32 devices in a mesh: blk: 8 (over z, y), off: 4 (over x, core).
Axes of the slice: x: 2, y: 2, z: 4, core: 2. Of those that a mesh axis runs over, the one named last changes fastest.
Arguments:
- orbitals: bfloat16 [8, 48, 2304], P('blk'), may hold values from -1.5 to 1.5
Outputs:
- exchange: float32 [8, 48, 2304], P('blk', 'off')
The draws below stay inside these ranges and needn't reach their ends.
All inputs are finite; a program needn't handle non-finite values.
Results may differ from the reference program's by a relative error of at most 0.00055.
Values may be sent and summed in bfloat16 or wider, within the bound.
No kernel may reach another device: no remote copies, remote signals or barrier semaphores. Data moves between devices by JAX's collectives and lax.ppermute only.
A program may use at most 64 MiB of HBM per device.

```python
import math
import jax
import jax.numpy as jnp
from jax import lax

NG = 48
BANDS = 8


def steps_of(rng, shape, split, smallest, top_value):
    gain = 1.0
    for dim, parts in split:
        draws = jax.random.uniform(jax.random.fold_in(jax.random.fold_in(rng, 6), dim), (parts,), jnp.float32, smallest / len(split), top_value / len(split))
        gain = gain * jnp.repeat(jnp.exp(draws), shape[dim] // parts).reshape((-1,) + (1,) * (len(shape) - 1 - dim))
    return gain


def gaussian(own_key, dims, scale, bound, split=(), held_as=jnp.bfloat16):
    loudness = steps_of(own_key, dims, split, -0.22, 0.18) if split else 1.0
    drawn = jax.random.normal(own_key, dims, jnp.float32) * scale * loudness
    return jnp.minimum(jnp.maximum(drawn, -bound), bound).astype(held_as)


def setup_inputs(seed: int = 0) -> dict:
    keys = jax.random.split(jax.random.key(seed), 2)
    orbitals = gaussian(keys[0], (BANDS, NG, NG * NG), 0.25, 1.5, ((0, 8),))
    return dict(orbitals=orbitals)


cell_edge = 59.0
screen_rate = 0.106


def screened_kernel(grid_edge):
    points = jnp.arange(grid_edge, dtype=jnp.int32)
    signed = jnp.where(points > grid_edge // 2, points - grid_edge, points)
    half_points = jnp.arange(grid_edge // 2 + 1, dtype=jnp.int32)
    squared = signed[:, None, None] ** 2 + signed[None, :, None] ** 2 + half_points[None, None, :] ** 2
    wave_sq = squared.astype(jnp.float32) * jnp.float32((2.0 * math.pi / cell_edge) ** 2)
    safe_sq = jnp.where(squared == 0, jnp.float32(1.0), wave_sq)
    screened = 4.0 * math.pi * (-jnp.expm1(-safe_sq / (4.0 * screen_rate ** 2))) / safe_sq
    return jnp.where(squared == 0, jnp.float32(math.pi / screen_rate ** 2), screened).astype(jnp.float32)


def reference(orbitals):
    fields = orbitals.astype(jnp.float32).reshape(BANDS, NG, NG, NG)
    kernel = screened_kernel(NG)

    def one_band(single):
        density = single[None] * fields
        spectrum = jnp.fft.rfftn(density, axes=(1, 2, 3))
        potential = jnp.fft.irfftn(spectrum * kernel, s=(NG, NG, NG), axes=(1, 2, 3))
        summed = -0.25 * jnp.sum(fields * potential, axis=0)
        return summed.reshape(NG, NG * NG).astype(jnp.float32)

    return lax.map(one_band, fields)
```

```python
import functools
import math

import jax
import jax.numpy as jnp
import numpy as np
from jax import lax
from jax.experimental import pallas as pl
from jax.experimental.pallas import tpu as pltpu
from jax.sharding import PartitionSpec as P

cell_edge = 59.0
screen_rate = 0.106
lanes = 128
half = lanes // 2


def signed_points(grid_edge):
    points = np.arange(grid_edge)
    return np.where(points > grid_edge // 2, points - grid_edge, points)


def real_basis(grid_edge):
    points = np.arange(grid_edge)
    angles = 2.0 * np.pi / grid_edge * (points[:, None] * points[None, :] % grid_edge)
    rows = np.where(points[:, None] <= grid_edge // 2, np.cos(angles), np.sin(angles))
    single = (points == 0) | (2 * points == grid_edge)
    return rows * np.sqrt(np.where(single, 1.0, 2.0) / grid_edge)[:, None]


def in_two(values):
    high = values.astype(jnp.bfloat16)
    low = (values - high.astype(np.float64)).astype(jnp.bfloat16)
    return high, low


def left_table(matrix):
    high, low = in_two(matrix)
    return np.concatenate([high, high, low], axis=1)


def right_table(matrix):
    edge = matrix.shape[0]
    both = np.zeros((lanes, lanes))
    both[:edge, :edge] = matrix
    both[half : half + edge, half : half + edge] = matrix
    high, low = in_two(both)
    return np.block([[high, low], [high, np.zeros_like(low)]])


def screened_kernel(grid_edge):
    signed = signed_points(grid_edge)
    row = np.zeros(lanes, np.int32)
    row[:grid_edge] = signed**2
    row[half : half + grid_edge] = signed**2
    squares = jnp.asarray(signed**2, jnp.int32)
    squared = squares[:, None, None] + squares[None, :, None] + jnp.asarray(row)[None, None, :]
    wave_sq = squared.astype(jnp.float32) * jnp.float32((2.0 * math.pi / cell_edge) ** 2)
    safe_sq = jnp.where(squared == 0, jnp.float32(1.0), wave_sq)
    screened = 4.0 * math.pi * -jnp.expm1(-safe_sq / (4.0 * screen_rate**2)) / safe_sq
    return jnp.where(squared == 0, jnp.float32(math.pi / screen_rate**2), screened)


def split(values):
    high = values.astype(jnp.bfloat16)
    low = (values - high.astype(jnp.float32)).astype(jnp.bfloat16)
    return high, low


def dot(left, right):
    return jnp.dot(left, right, preferred_element_type=jnp.float32)


def rows_transform(table, slabs):
    done = []
    for first in range(0, len(slabs), 2):
        columns = []
        for slab in slabs[first : first + 2]:
            high, low = split(slab)
            columns.append(jnp.concatenate([high, low, high], axis=0))
        product = dot(table, jnp.concatenate(columns, axis=1))
        for k in range(len(columns)):
            done.append(product[:, k * lanes : (k + 1) * lanes])
    return done


def lanes_transform(slabs, table):
    edge = slabs[0].shape[0]
    high, low = split(jnp.concatenate(slabs, axis=0))
    product = dot(jnp.concatenate([high, low], axis=1), table)
    product = product[:, :lanes] + product[:, lanes:]
    return [product[k * edge : (k + 1) * edge] for k in range(len(slabs))]


def pair_kernel(
    grid_edge, slots, order_ref, home_ref, ahead_ref, behind_ref, kernel_ref,
    left_fwd_ref, left_back_ref, right_fwd_ref, right_back_ref, near_ref, far_ref, work, result,
):
    group = lanes // math.gcd(lanes, grid_edge)
    width = group * grid_edge
    tiles = width // lanes
    planes = grid_edge // slots
    lane = lax.broadcasted_iota(jnp.int32, (grid_edge, lanes), 1)

    def tiles_of(ref, start):
        return [
            ref[:, pl.ds(pl.multiple_of(start + t * lanes, lanes), lanes)].astype(jnp.float32)
            for t in range(tiles)
        ]

    def turn(values, amount):
        amount %= lanes
        return pltpu.roll(values, amount, 1) if amount else values

    @pl.loop(0, grid_edge // group)
    def _(block):
        start = block * width
        home = tiles_of(home_ref, start)
        first = [a * b for a, b in zip(home, tiles_of(ahead_ref, start))]
        second = [turn(a * b, half) for a, b in zip(home, tiles_of(behind_ref, start))]
        slabs = []
        for k in range(group):
            tile, offset = divmod(k * grid_edge, lanes)
            in_first = ((lane + (lanes - offset)) % lanes) < half
            this_a, this_b = first[tile], second[tile]
            if offset + grid_edge > lanes:
                this_a = jnp.where(lane >= offset, this_a, first[tile + 1])
                from_this = ((lane + half) % lanes) >= offset
                this_b = jnp.where(from_this, this_b, second[tile + 1])
            slabs.append(turn(jnp.where(in_first, this_a, this_b), -offset))
        slabs = lanes_transform(slabs, right_fwd_ref[...])
        slabs = rows_transform(left_fwd_ref[...], slabs)
        for k, slab in enumerate(slabs):
            at = pl.multiple_of((block * group + k) * grid_edge, grid_edge)
            work[pl.ds(at, grid_edge), :] = slab

    together = 8 if grid_edge % 8 == 0 else 1

    @pl.loop(0, grid_edge // together)
    def _(block):
        rows = [pl.ds(block * together + k, grid_edge, stride=grid_edge) for k in range(together)]
        slabs = rows_transform(left_fwd_ref[...], [work[r, :] for r in rows])
        slabs = [slab * kernel_ref[block * together + k] for k, slab in enumerate(slabs)]
        slabs = rows_transform(left_back_ref[...], slabs)
        for r, slab in zip(rows, slabs):
            work[r, :] = slab

    @pl.loop(0, grid_edge // group)
    def _(block):
        start = block * width
        slabs = []
        for k in range(group):
            at = pl.multiple_of((block * group + k) * grid_edge, grid_edge)
            slabs.append(work[pl.ds(at, grid_edge), :])
        slabs = rows_transform(left_back_ref[...], slabs)
        slabs = lanes_transform(slabs, right_back_ref[...])
        slabs = [turn(slab, k * grid_edge) for k, slab in enumerate(slabs)]
        ahead = tiles_of(ahead_ref, start)
        behind = tiles_of(behind_ref, start)
        for t in range(tiles):
            sources = range(t * lanes // grid_edge, ((t + 1) * lanes - 1) // grid_edge + 1)
            dense_a = dense_b = slabs[sources[0]]
            shifted = (lane + half) % lanes
            for k in sources[1:]:
                edge_lane = k * grid_edge - t * lanes
                dense_a = jnp.where(lane >= edge_lane, slabs[k], dense_a)
                dense_b = jnp.where(shifted >= edge_lane, slabs[k], dense_b)
            total = -0.25 * (dense_a * ahead[t] + turn(dense_b, half) * behind[t])
            columns = pl.ds(pl.multiple_of(start + t * lanes, lanes), lanes)
            for p in range(slots):
                result[order_ref[p], :, columns] = total[p * planes : (p + 1) * planes]

    for k in range(slots // 2):
        near_ref[k] = result[2 * k]
        far_ref[k] = result[2 * k + 1]


def pair_terms(order, home, ahead, behind, kernel):
    grid_edge, plane_size = home.shape
    slots = order.shape[0]
    basis = real_basis(grid_edge)
    tables = (left_table(basis), left_table(basis.T), right_table(basis.T), right_table(basis))
    part = jax.ShapeDtypeStruct((slots // 2, grid_edge // slots, plane_size), jnp.float32)
    vmem = pl.BlockSpec(memory_space=pltpu.VMEM)
    return pl.pallas_call(
        functools.partial(pair_kernel, grid_edge, slots),
        out_shape=(part, part),
        in_specs=[pl.BlockSpec(memory_space=pltpu.SMEM)] + [vmem] * 8,
        out_specs=(vmem, vmem),
        scratch_shapes=[
            pltpu.VMEM((grid_edge * grid_edge, lanes), jnp.float32),
            pltpu.VMEM((slots, grid_edge // slots, plane_size), jnp.float32),
        ],
        compiler_params=pltpu.CompilerParams(vmem_limit_bytes=32 * 1024 * 1024),
        cost_estimate=pl.CostEstimate(flops=2 * 10**9, bytes_accessed=3 * 10**6, transcendentals=0),
    )(order, home, ahead, behind, kernel, *(jnp.asarray(t) for t in tables))


def offsets_of(cycle_size, groups):
    bits = groups.bit_length() - 1
    turned = [int(format(g, "b").zfill(bits)[::-1], 2) if bits else 0 for g in range(groups)]
    ahead = [d if d else cycle_size // 2 for d in turned]
    behind = [-d for d in turned]
    return ahead, behind


def fetch(block, offsets, cycle_size, groups):
    route = []
    for blk in range(cycle_size):
        for g in range(groups):
            if offsets[g] % cycle_size:
                route.append(((blk + offsets[g]) % cycle_size * groups + g, blk * groups + g))
    return lax.ppermute(block, ("blk", "off"), route)


def scattered_sum(near, far, groups):
    bit = 1
    while True:
        arrived = lax.ppermute(far, "off", [(g, g ^ bit) for g in range(groups)])
        near = near + arrived
        bit *= 2
        if bit == groups:
            return near[0]
        near, far = near[0::2], near[1::2]


def on_device(orbitals):
    band_count, grid_edge, plane_size = orbitals.shape
    cycle_size, groups = lax.axis_size("blk"), lax.axis_size("off")
    if cycle_size != 2 * groups or groups & (groups - 1) or groups < 2:
        raise ValueError("unsupported mesh")
    me = lax.axis_index("off")
    ahead_offsets, behind_offsets = offsets_of(cycle_size, groups)
    behind = fetch(orbitals, behind_offsets, cycle_size, groups)
    ahead = fetch(orbitals, ahead_offsets, cycle_size, groups)
    behind = jnp.where(me == 0, orbitals, behind)
    kernel = screened_kernel(grid_edge)
    order = jnp.arange(groups, dtype=jnp.int32) ^ me
    rows = []
    for i in range(band_count):
        near = far = 0.0
        for j in range(band_count):
            terms = pair_terms(order, orbitals[i], ahead[j], behind[j], kernel)
            near, far = near + terms[0], far + terms[1]
        rows.append(scattered_sum(near, far, groups))
    return jnp.stack(rows)


def solution(mesh):
    return jax.shard_map(
        on_device,
        mesh=mesh,
        in_specs=(P("blk", None, None),),
        out_specs=P("blk", "off", None),
        check_vma=False,
    )
```

```python
import functools
import math

import jax
import jax.numpy as jnp
import numpy as np
from jax import lax
from jax.experimental import pallas as pl
from jax.experimental.pallas import tpu as pltpu
from jax.sharding import PartitionSpec as P

cell_edge = 59.0
screen_rate = 0.106
lanes = 128
half = lanes // 2


def signed_points(grid_edge):
    points = np.arange(grid_edge)
    return np.where(points > grid_edge // 2, points - grid_edge, points)


def real_basis(grid_edge):
    points = np.arange(grid_edge)
    angles = 2.0 * np.pi / grid_edge * (points[:, None] * points[None, :] % grid_edge)
    rows = np.where(points[:, None] <= grid_edge // 2, np.cos(angles), np.sin(angles))
    single = (points == 0) | (2 * points == grid_edge)
    return rows * np.sqrt(np.where(single, 1.0, 2.0) / grid_edge)[:, None]


def in_two(values):
    high = values.astype(jnp.bfloat16)
    low = (values - high.astype(np.float64)).astype(jnp.bfloat16)
    return high, low


def left_table(matrix):
    high, low = in_two(matrix)
    return np.concatenate([high, high, low], axis=1)


def right_table(matrix):
    edge = matrix.shape[0]
    both = np.zeros((lanes, lanes))
    both[:edge, :edge] = matrix
    both[half : half + edge, half : half + edge] = matrix
    high, low = in_two(both)
    return np.block([[high, low], [high, np.zeros_like(low)]])


def screened_kernel(grid_edge):
    signed = signed_points(grid_edge)
    row = np.zeros(lanes, np.int32)
    row[:grid_edge] = signed**2
    row[half : half + grid_edge] = signed**2
    squares = jnp.asarray(signed**2, jnp.int32)
    squared = squares[:, None, None] + squares[None, :, None] + jnp.asarray(row)[None, None, :]
    wave_sq = squared.astype(jnp.float32) * jnp.float32((2.0 * math.pi / cell_edge) ** 2)
    safe_sq = jnp.where(squared == 0, jnp.float32(1.0), wave_sq)
    screened = 4.0 * math.pi * -jnp.expm1(-safe_sq / (4.0 * screen_rate**2)) / safe_sq
    return jnp.where(squared == 0, jnp.float32(math.pi / screen_rate**2), screened)


def split(values):
    high = values.astype(jnp.bfloat16)
    low = (values - high.astype(jnp.float32)).astype(jnp.bfloat16)
    return high, low


def dot(left, right):
    return jnp.dot(left, right, preferred_element_type=jnp.float32)


def rows_transform(table, slabs):
    done = []
    for first in range(0, len(slabs), 2):
        columns = []
        for slab in slabs[first : first + 2]:
            high, low = split(slab)
            columns.append(jnp.concatenate([high, low, high], axis=0))
        product = dot(table, jnp.concatenate(columns, axis=1))
        for k in range(len(columns)):
            done.append(product[:, k * lanes : (k + 1) * lanes])
    return done


def lanes_transform(slabs, table):
    edge = slabs[0].shape[0]
    high, low = split(jnp.concatenate(slabs, axis=0))
    product = dot(jnp.concatenate([high, low], axis=1), table)
    product = product[:, :lanes] + product[:, lanes:]
    return [product[k * edge : (k + 1) * edge] for k in range(len(slabs))]


def pair_kernel(
    grid_edge, slots, order_ref, home_ref, ahead_ref, behind_ref, kernel_ref,
    left_fwd_ref, left_back_ref, right_fwd_ref, right_back_ref, near_ref, far_ref, work, back, result,
):
    group = lanes // math.gcd(lanes, grid_edge)
    tiles = group * grid_edge // lanes
    pitch = work.shape[0] // grid_edge
    planes = grid_edge // slots
    row_tiles = grid_edge * grid_edge // lanes
    lane = lax.broadcasted_iota(jnp.int32, (grid_edge, lanes), 1)
    shifted = (lane + half) % lanes

    def tiles_of(ref, block):
        first = block * tiles
        return [
            ref[:, (first + t) * lanes : (first + t + 1) * lanes].astype(jnp.float32)
            for t in range(tiles)
        ]

    def turn(values, amount):
        amount %= lanes
        return pltpu.roll(values, amount, 1) if amount else values

    for block in range(grid_edge // group):
        home = tiles_of(home_ref, block)
        first = [a * b for a, b in zip(home, tiles_of(ahead_ref, block))]
        second = [turn(a * b, half) for a, b in zip(home, tiles_of(behind_ref, block))]
        slabs = []
        for k in range(group):
            tile, offset = divmod(k * grid_edge, lanes)
            in_first = ((lane + (lanes - offset)) % lanes) < half
            this_a, this_b = first[tile], second[tile]
            if offset + grid_edge > lanes:
                this_a = jnp.where(lane >= offset, this_a, first[tile + 1])
                this_b = jnp.where(shifted >= offset, this_b, second[tile + 1])
            slabs.append(turn(jnp.where(in_first, this_a, this_b), -offset))
        slabs = lanes_transform(slabs, right_fwd_ref[...])
        slabs = rows_transform(left_fwd_ref[...], slabs)
        for k, slab in enumerate(slabs):
            work[pl.ds((block * group + k) * pitch, grid_edge), :] = slab

    for block in range(grid_edge // group):
        rows = [pl.ds(block * group + k, grid_edge, stride=pitch) for k in range(group)]
        slabs = rows_transform(left_fwd_ref[...], [work[r, :] for r in rows])
        slabs = [slab * kernel_ref[block * group + k] for k, slab in enumerate(slabs)]
        slabs = rows_transform(left_back_ref[...], slabs)
        for r, slab in zip(rows, slabs):
            back[r, :] = slab

    for block in range(grid_edge // group):
        slabs = [back[pl.ds((block * group + k) * pitch, grid_edge), :] for k in range(group)]
        slabs = rows_transform(left_back_ref[...], slabs)
        slabs = lanes_transform(slabs, right_back_ref[...])
        slabs = [turn(slab, k * grid_edge) for k, slab in enumerate(slabs)]
        ahead = tiles_of(ahead_ref, block)
        behind = tiles_of(behind_ref, block)
        for t in range(tiles):
            sources = range(t * lanes // grid_edge, ((t + 1) * lanes - 1) // grid_edge + 1)
            dense_a = dense_b = slabs[sources[0]]
            for k in sources[1:]:
                edge_lane = k * grid_edge - t * lanes
                dense_a = jnp.where(lane >= edge_lane, slabs[k], dense_a)
                dense_b = jnp.where(shifted >= edge_lane, slabs[k], dense_b)
            total = -0.25 * (dense_a * ahead[t] + turn(dense_b, half) * behind[t])
            rows = pl.ds(block * tiles + t, planes, stride=row_tiles)
            for p in range(slots):
                result[order_ref[p], rows, :] = total[p * planes : (p + 1) * planes]

    for k in range(slots // 2):
        near_ref[k] = result[2 * k]
        far_ref[k] = result[2 * k + 1]


def pair_terms(order, home, ahead, behind, kernel):
    grid_edge, plane_size = home.shape
    slots = order.shape[0]
    basis = real_basis(grid_edge)
    tables = (left_table(basis), left_table(basis.T), right_table(basis.T), right_table(basis))
    slot_rows = grid_edge // slots * plane_size // lanes
    pitch = -(-grid_edge // 8) * 8 + 4
    part = jax.ShapeDtypeStruct((slots // 2, slot_rows, lanes), jnp.float32)
    vmem = pl.BlockSpec(memory_space=pltpu.VMEM)
    return pl.pallas_call(
        functools.partial(pair_kernel, grid_edge, slots),
        out_shape=(part, part),
        in_specs=[pl.BlockSpec(memory_space=pltpu.SMEM)] + [vmem] * 8,
        out_specs=(vmem, vmem),
        scratch_shapes=[
            pltpu.VMEM((grid_edge * pitch, lanes), jnp.float32),
            pltpu.VMEM((grid_edge * pitch, lanes), jnp.float32),
            pltpu.VMEM((slots, slot_rows, lanes), jnp.float32),
        ],
        compiler_params=pltpu.CompilerParams(vmem_limit_bytes=32 * 1024 * 1024),
        cost_estimate=pl.CostEstimate(flops=2 * 10**9, bytes_accessed=3 * 10**6, transcendentals=0),
    )(order, home, ahead, behind, kernel, *(jnp.asarray(t) for t in tables))


def offsets_of(cycle_size, groups):
    bits = groups.bit_length() - 1
    turned = [int(format(g, "b").zfill(bits)[::-1], 2) if bits else 0 for g in range(groups)]
    ahead = [d if d else cycle_size // 2 for d in turned]
    behind = [-d for d in turned]
    return ahead, behind


def fetch(block, offsets, cycle_size, groups):
    route = []
    for blk in range(cycle_size):
        for g in range(groups):
            if offsets[g] % cycle_size:
                route.append(((blk + offsets[g]) % cycle_size * groups + g, blk * groups + g))
    return lax.ppermute(block, ("blk", "off"), route)


def scattered_sum(near, far, groups):
    bit = 1
    while True:
        arrived = lax.ppermute(far, "off", [(g, g ^ bit) for g in range(groups)])
        near = near + arrived
        bit *= 2
        if bit == groups:
            return near[0]
        near, far = near[0::2], near[1::2]


def on_device(orbitals):
    band_count, grid_edge, plane_size = orbitals.shape
    cycle_size, groups = lax.axis_size("blk"), lax.axis_size("off")
    if cycle_size != 2 * groups or groups & (groups - 1) or groups < 2 or grid_edge > half:
        raise ValueError("unsupported mesh")
    me = lax.axis_index("off")
    ahead_offsets, behind_offsets = offsets_of(cycle_size, groups)
    behind = fetch(orbitals, behind_offsets, cycle_size, groups)
    ahead = fetch(orbitals, ahead_offsets, cycle_size, groups)
    behind = jnp.where(me == 0, orbitals, behind)
    kernel = screened_kernel(grid_edge)
    order = jnp.arange(groups, dtype=jnp.int32) ^ me
    rows = []
    for i in range(band_count):
        near = far = 0.0
        for j in range(band_count):
            terms = pair_terms(order, orbitals[i], ahead[j], behind[j], kernel)
            near, far = near + terms[0], far + terms[1]
        rows.append(scattered_sum(near, far, groups))
    return jnp.stack(rows).reshape(band_count, grid_edge // groups, plane_size)


def solution(mesh):
    return jax.shard_map(
        on_device,
        mesh=mesh,
        in_specs=(P("blk", None, None),),
        out_specs=P("blk", "off", None),
        check_vma=False,
    )
```

```python
import functools
import math

import jax
import jax.numpy as jnp
import numpy as np
from jax import lax
from jax.experimental import pallas as pl
from jax.experimental.pallas import tpu as pltpu
from jax.sharding import PartitionSpec as P

cell_edge = 59.0
screen_rate = 0.106
lanes = 128
together_blocks = 2
half = lanes // 2


def signed_points(grid_edge):
    points = np.arange(grid_edge)
    return np.where(points > grid_edge // 2, points - grid_edge, points)


def real_basis(grid_edge):
    points = np.arange(grid_edge)
    angles = 2.0 * np.pi / grid_edge * (points[:, None] * points[None, :] % grid_edge)
    rows = np.where(points[:, None] <= grid_edge // 2, np.cos(angles), np.sin(angles))
    single = (points == 0) | (2 * points == grid_edge)
    return rows * np.sqrt(np.where(single, 1.0, 2.0) / grid_edge)[:, None]


def in_two(values):
    high = values.astype(jnp.bfloat16)
    low = (values - high.astype(np.float64)).astype(jnp.bfloat16)
    return high, low


def left_table(matrix):
    high, low = in_two(matrix)
    return np.concatenate([high, high, low], axis=1)


def right_table(matrix, start_in, start_out):
    edge = matrix.shape[0]
    both = np.zeros((lanes, lanes))
    both[:edge, :edge] = matrix
    both[start_in : start_in + edge, start_out : start_out + edge] = matrix
    high, low = in_two(both)
    return np.block([[high, low], [high, np.zeros_like(low)]])


def screened_kernel(grid_edge):
    signed = signed_points(grid_edge)
    row = np.zeros(lanes, np.int32)
    row[:grid_edge] = signed**2
    row[half : half + grid_edge] = signed**2
    pair = np.where(np.arange(lanes) < half, signed[0::2, None] ** 2, signed[1::2, None] ** 2) + row
    squared = jnp.asarray(pair, jnp.int32)[:, None, :] + jnp.asarray(signed**2, jnp.int32)[None, :, None]
    wave_sq = squared.astype(jnp.float32) * jnp.float32((2.0 * math.pi / cell_edge) ** 2)
    safe_sq = jnp.where(squared == 0, jnp.float32(1.0), wave_sq)
    screened = 4.0 * math.pi * -jnp.expm1(-safe_sq / (4.0 * screen_rate**2)) / safe_sq
    return jnp.where(squared == 0, jnp.float32(math.pi / screen_rate**2), screened)


def split(values):
    high = values.astype(jnp.bfloat16)
    low = (values - high.astype(jnp.float32)).astype(jnp.bfloat16)
    return high, low


def dot(left, right):
    return jnp.dot(left, right, preferred_element_type=jnp.float32)


def rows_products(table, slabs):
    done = []
    for first in range(0, len(slabs), 2):
        columns = []
        for slab in slabs[first : first + 2]:
            high, low = split(slab)
            columns.append(jnp.concatenate([high, low, high], axis=0))
        product = dot(table, jnp.concatenate(columns, axis=1))
        done += [product[:, k * lanes : (k + 1) * lanes] for k in range(len(columns))]
    return done


def lanes_product(slabs, table):
    high, low = split(jnp.concatenate(slabs, axis=0))
    return dot(jnp.concatenate([high, low], axis=1), table)


def lanes_result(product, count):
    edge = product.shape[0] // count
    product = product[:, :lanes] + product[:, lanes:]
    return [product[k * edge : (k + 1) * edge] for k in range(count)]


def in_steps(count, *steps):
    held = [{} for _ in steps]
    for time in range(count + len(steps) - 1):
        for n, step in enumerate(steps):
            item = time - n
            if 0 <= item < count:
                given = (held[n - 1].pop(item),) if n else ()
                held[n][item] = step(item, *given)


def pair_kernel(grid_edge, slots, has_prior, last, *refs):
    refs = list(refs)
    order_ref, home_ref, other_ref, kernel_ref = refs[:4]
    left_first_ref, left_fwd_ref, left_back_ref, left_last_ref, right_fwd_ref, right_back_ref = refs[4:10]
    prior_ref = refs[10] if has_prior else None
    outs = refs[10 + has_prior : -2 - last]
    work, back = refs[-2 - last], refs[-1 - last]
    result = refs[-1] if last else outs[0]

    line = 2 * grid_edge
    group = lanes // math.gcd(lanes, line)
    tiles = group * line // lanes
    pitch = work.shape[0] // (grid_edge // 2)
    planes = grid_edge // slots
    row_tiles = grid_edge * grid_edge // lanes
    lane = lax.broadcasted_iota(jnp.int32, (grid_edge, lanes), 1)
    together = together_blocks if grid_edge % (2 * together_blocks) == 0 else 1
    in_first = lax.broadcasted_iota(jnp.int32, (grid_edge // 2, lanes), 1) < half

    def tiles_of(ref, block):
        first = block * tiles
        return [
            ref[:, (first + t) * lanes : (first + t + 1) * lanes].astype(jnp.float32)
            for t in range(tiles)
        ]

    def turn(values, amount):
        amount %= lanes
        return pltpu.roll(values, amount, 1) if amount else values

    def first_lanes(block):
        dense = [a * b for a, b in zip(tiles_of(home_ref, block), tiles_of(other_ref, block))]
        slabs = []
        for k in range(group):
            tile, offset = divmod(k * line, lanes)
            slab = dense[tile]
            if offset + line > lanes:
                slab = jnp.where(lane >= offset, slab, dense[tile + 1])
            slabs.append(turn(slab, -offset))
        return lanes_product(slabs, right_fwd_ref[...])

    def first_rows(block, product):
        return rows_products(left_first_ref[...], lanes_result(product, group))

    def first_store(block, slabs):
        for k, slab in enumerate(slabs):
            work[pl.ds((block * group + k) * pitch, grid_edge), :] = slab

    in_steps(grid_edge // 2 // group, first_lanes, first_rows, first_store)

    def rows_of(block):
        start = 2 * block * together
        return [
            [pl.ds(start + 2 * k + d, grid_edge // 2, stride=pitch) for d in range(2)]
            for k in range(together)
        ]

    def middle_forward(block):
        slabs = []
        for pair in rows_of(block):
            even, odd = (work[r, :] for r in pair)
            top = jnp.where(in_first, even, turn(odd, half))
            bottom = jnp.where(in_first, turn(even, half), odd)
            slabs.append(jnp.concatenate([top, bottom], axis=0))
        return rows_products(left_fwd_ref[...], slabs)

    def middle_back(block, slabs):
        slabs = [slab * kernel_ref[block * together + k] for k, slab in enumerate(slabs)]
        return rows_products(left_back_ref[...], slabs)

    def middle_store(block, slabs):
        for (row_even, row_odd), slab in zip(rows_of(block), slabs):
            top, bottom = slab[: grid_edge // 2], slab[grid_edge // 2 :]
            back[row_even, :] = jnp.where(in_first, top, turn(bottom, half))
            back[row_odd, :] = jnp.where(in_first, turn(top, half), bottom)

    in_steps(grid_edge // 2 // together, middle_forward, middle_back, middle_store)

    def last_rows(block):
        slabs = [back[pl.ds((block * group + k) * pitch, grid_edge), :] for k in range(group)]
        return rows_products(left_last_ref[...], slabs)

    def last_lanes(block, slabs):
        return lanes_product(slabs, right_back_ref[...])

    def last_store(block, product):
        slabs = [turn(slab, k * line) for k, slab in enumerate(lanes_result(product, group))]
        other = tiles_of(other_ref, block)
        for t in range(tiles):
            sources = range(t * lanes // line, ((t + 1) * lanes - 1) // line + 1)
            dense = slabs[sources[0]]
            for k in sources[1:]:
                dense = jnp.where(lane >= k * line - t * lanes, slabs[k], dense)
            total = -0.25 * (dense * other[t])
            rows = pl.ds(block * tiles + t, planes, stride=row_tiles)
            for p in range(slots):
                result[order_ref[p], rows, :] = total[p * planes : (p + 1) * planes]

    in_steps(grid_edge // 2 // group, last_rows, last_lanes, last_store)

    if last:
        for k in range(slots):
            terms = result[k]
            if has_prior:
                terms += prior_ref[k]
            outs[k % 2][k // 2] = terms
    elif has_prior:
        result[...] += prior_ref[...]


def pair_terms(order, home, other, kernel, prior, last):
    grid_edge, plane_size = home.shape
    slots = order.shape[0]
    basis = real_basis(grid_edge)
    mixed = np.concatenate([np.arange(0, grid_edge, 2), np.arange(1, grid_edge, 2)])
    tables = (
        left_table(basis),
        left_table(basis[:, mixed]),
        left_table(basis.T[mixed]),
        left_table(basis.T),
        right_table(basis.T, grid_edge, half),
        right_table(basis, half, grid_edge),
    )
    slot_rows = grid_edge // slots * plane_size // lanes
    pitch = -(-grid_edge // 8) * 8 + 4
    whole = jax.ShapeDtypeStruct((slots, slot_rows, lanes), jnp.float32)
    part = jax.ShapeDtypeStruct((slots // 2, slot_rows, lanes), jnp.float32)
    vmem = pl.BlockSpec(memory_space=pltpu.VMEM)
    operands = [order, home, other, kernel, *(jnp.asarray(t) for t in tables)]
    operands += [] if prior is None else [prior]
    scratch = [pltpu.VMEM((grid_edge // 2 * pitch, lanes), jnp.float32)] * 2
    scratch += [pltpu.VMEM(whole.shape, jnp.float32)] if last else []
    return pl.pallas_call(
        functools.partial(pair_kernel, grid_edge, slots, prior is not None, last),
        out_shape=(part, part) if last else whole,
        in_specs=[pl.BlockSpec(memory_space=pltpu.SMEM)] + [vmem] * (len(operands) - 1),
        out_specs=(vmem, vmem) if last else vmem,
        scratch_shapes=scratch,
        compiler_params=pltpu.CompilerParams(vmem_limit_bytes=32 * 1024 * 1024),
        cost_estimate=pl.CostEstimate(flops=10**9, bytes_accessed=2 * 10**6, transcendentals=0),
    )(*operands)


def fetch(block, masks, cycle_size, groups):
    route = []
    for blk in range(cycle_size):
        for g in range(groups):
            if masks[g]:
                route.append(((blk ^ masks[g]) * groups + g, blk * groups + g))
    return lax.ppermute(block, ("blk", "off"), route)


def scattered_sum(near, far, groups):
    bit = 1
    while True:
        arrived = lax.ppermute(far, "off", [(g, g ^ bit) for g in range(groups)])
        near = near + arrived
        bit *= 2
        if bit == groups:
            return near[0]
        near, far = near[0::2], near[1::2]


def on_device(orbitals):
    band_count, grid_edge, plane_size = orbitals.shape
    cycle_size, groups = lax.axis_size("blk"), lax.axis_size("off")
    if cycle_size != 2 * groups or groups & (groups - 1) or groups < 2 or grid_edge > half:
        raise ValueError("unsupported mesh")
    me = lax.axis_index("off")
    early = fetch(orbitals, list(range(groups)), cycle_size, groups)
    late = fetch(orbitals, list(range(groups, cycle_size)), cycle_size, groups)
    early = jnp.where(me == 0, orbitals, early)
    kernel = screened_kernel(grid_edge)
    order = jnp.arange(groups, dtype=jnp.int32) ^ me
    rows = []
    for home in orbitals:
        others = [*early, *late]
        terms = None
        for other in others[:-1]:
            terms = pair_terms(order, home, other, kernel, terms, False)
        near, far = pair_terms(order, home, others[-1], kernel, terms, True)
        rows.append(scattered_sum(near, far, groups))
    return jnp.stack(rows).reshape(band_count, grid_edge // groups, plane_size)


def solution(mesh):
    return jax.shard_map(
        on_device,
        mesh=mesh,
        in_specs=(P("blk", None, None),),
        out_specs=P("blk", "off", None),
        check_vma=False,
    )
```

```python
import functools
import math

import jax
import jax.numpy as jnp
import numpy as np
from jax import lax
from jax.experimental import pallas as pl
from jax.experimental.pallas import tpu as pltpu
from jax.sharding import PartitionSpec as P


cell_edge = 59.0
screen_rate = 0.106
lanes = 128
together_blocks = 2
half = lanes // 2


def signed_points(grid_edge):
    points = np.arange(grid_edge)
    return np.where(points > grid_edge // 2, points - grid_edge, points)


def real_basis(grid_edge):
    points = np.arange(grid_edge)
    angles = 2.0 * np.pi / grid_edge * (points[:, None] * points[None, :] % grid_edge)
    rows = np.where(points[:, None] <= grid_edge // 2, np.cos(angles), np.sin(angles))
    single = (points == 0) | (2 * points == grid_edge)
    return rows * np.sqrt(np.where(single, 1.0, 2.0) / grid_edge)[:, None]


def in_two(values):
    high = values.astype(jnp.bfloat16)
    low = (values - high.astype(np.float64)).astype(jnp.bfloat16)
    return high, low


def left_table(matrix):
    high, low = in_two(matrix)
    return np.concatenate([high, high, low], axis=1)


def right_table(matrix, start_in, start_out):
    edge = matrix.shape[0]
    both = np.zeros((lanes, lanes))
    both[:edge, :edge] = matrix
    both[start_in : start_in + edge, start_out : start_out + edge] = matrix
    high, low = in_two(both)
    return np.block([[high, low], [high, np.zeros_like(low)]])


def screened_kernel(grid_edge):
    signed = signed_points(grid_edge)
    row = np.zeros(lanes, np.int32)
    row[:grid_edge] = signed**2
    row[half : half + grid_edge] = signed**2
    pair = np.where(np.arange(lanes) < half, signed[0::2, None] ** 2, signed[1::2, None] ** 2) + row
    squared = jnp.asarray(pair, jnp.int32)[:, None, :] + jnp.asarray(signed**2, jnp.int32)[None, :, None]
    wave_sq = squared.astype(jnp.float32) * jnp.float32((2.0 * math.pi / cell_edge) ** 2)
    safe_sq = jnp.where(squared == 0, jnp.float32(1.0), wave_sq)
    screened = 4.0 * math.pi * -jnp.expm1(-safe_sq / (4.0 * screen_rate**2)) / safe_sq
    return jnp.where(squared == 0, jnp.float32(math.pi / screen_rate**2), screened)


def split(values):
    high = values.astype(jnp.bfloat16)
    low = (values - high.astype(jnp.float32)).astype(jnp.bfloat16)
    return high, low


def dot(left, right):
    return jnp.dot(left, right, preferred_element_type=jnp.float32)


def rows_products(table, slabs):
    done = []
    for first in range(0, len(slabs), 2):
        columns = []
        for slab in slabs[first : first + 2]:
            high, low = split(slab)
            columns.append(jnp.concatenate([high, low, high], axis=0))
        product = dot(table, jnp.concatenate(columns, axis=1))
        done += [product[:, k * lanes : (k + 1) * lanes] for k in range(len(columns))]
    return done


def lanes_product(slabs, table):
    high, low = split(jnp.concatenate(slabs, axis=0))
    return dot(jnp.concatenate([high, low], axis=1), table)


def lanes_result(product, count):
    edge = product.shape[0] // count
    product = product[:, :lanes] + product[:, lanes:]
    return [product[k * edge : (k + 1) * edge] for k in range(count)]


def in_steps(count, *steps):
    held = [{} for _ in steps]
    for time in range(count + len(steps) - 1):
        for n, step in enumerate(steps):
            item = time - n
            if 0 <= item < count:
                given = (held[n - 1].pop(item),) if n else ()
                held[n][item] = step(item, *given)


def pair_kernel(grid_edge, slots, has_prior, last, *refs):
    refs = list(refs)
    order_ref, home_ref, other_ref, kernel_ref = refs[:4]
    left_first_ref, left_fwd_ref, left_back_ref, left_last_ref, right_fwd_ref, right_back_ref = refs[4:10]
    prior_ref = refs[10] if has_prior else None
    outs = refs[10 + has_prior : -2 - last]
    work, back = refs[-2 - last], refs[-1 - last]
    result = refs[-1] if last else outs[0]

    line = 2 * grid_edge
    group = lanes // math.gcd(lanes, line)
    tiles = group * line // lanes
    pitch = work.shape[0] // (grid_edge // 2)
    planes = grid_edge // slots
    row_tiles = grid_edge * grid_edge // lanes
    lane = lax.broadcasted_iota(jnp.int32, (grid_edge, lanes), 1)
    together = together_blocks if grid_edge % (2 * together_blocks) == 0 else 1
    in_first = lax.broadcasted_iota(jnp.int32, (grid_edge // 2, lanes), 1) < half

    def tiles_of(ref, block):
        first = block * tiles
        return [
            ref[:, (first + t) * lanes : (first + t + 1) * lanes].astype(jnp.float32)
            for t in range(tiles)
        ]

    def turn(values, amount):
        amount %= lanes
        return pltpu.roll(values, amount, 1) if amount else values

    def first_lanes(block):
        dense = [a * b for a, b in zip(tiles_of(home_ref, block), tiles_of(other_ref, block))]
        slabs = []
        for k in range(group):
            tile, offset = divmod(k * line, lanes)
            slab = dense[tile]
            if offset + line > lanes:
                slab = jnp.where(lane >= offset, slab, dense[tile + 1])
            slabs.append(turn(slab, -offset))
        return lanes_product(slabs, right_fwd_ref[...])

    def first_rows(block, product):
        return rows_products(left_first_ref[...], lanes_result(product, group))

    def first_store(block, slabs):
        for k, slab in enumerate(slabs):
            work[pl.ds((block * group + k) * pitch, grid_edge), :] = slab

    in_steps(grid_edge // 2 // group, first_lanes, first_rows, first_store)

    def rows_of(block):
        start = 2 * block * together
        return [
            [pl.ds(start + 2 * k + d, grid_edge // 2, stride=pitch) for d in range(2)]
            for k in range(together)
        ]

    def middle_forward(block):
        slabs = []
        for pair in rows_of(block):
            even, odd = (work[r, :] for r in pair)
            top = jnp.where(in_first, even, turn(odd, half))
            bottom = jnp.where(in_first, turn(even, half), odd)
            slabs.append(jnp.concatenate([top, bottom], axis=0))
        return rows_products(left_fwd_ref[...], slabs)

    def middle_back(block, slabs):
        slabs = [slab * kernel_ref[block * together + k] for k, slab in enumerate(slabs)]
        return rows_products(left_back_ref[...], slabs)

    def middle_store(block, slabs):
        for (row_even, row_odd), slab in zip(rows_of(block), slabs):
            top, bottom = slab[: grid_edge // 2], slab[grid_edge // 2 :]
            back[row_even, :] = jnp.where(in_first, top, turn(bottom, half))
            back[row_odd, :] = jnp.where(in_first, turn(top, half), bottom)

    in_steps(grid_edge // 2 // together, middle_forward, middle_back, middle_store)

    def last_rows(block):
        slabs = [back[pl.ds((block * group + k) * pitch, grid_edge), :] for k in range(group)]
        return rows_products(left_last_ref[...], slabs)

    def last_lanes(block, slabs):
        return lanes_product(slabs, right_back_ref[...])

    def last_store(block, product):
        slabs = [turn(slab, k * line) for k, slab in enumerate(lanes_result(product, group))]
        other = tiles_of(other_ref, block)
        for t in range(tiles):
            sources = range(t * lanes // line, ((t + 1) * lanes - 1) // line + 1)
            dense = slabs[sources[0]]
            for k in sources[1:]:
                dense = jnp.where(lane >= k * line - t * lanes, slabs[k], dense)
            total = -0.25 * (dense * other[t])
            rows = pl.ds(block * tiles + t, planes, stride=row_tiles)
            for p in range(slots):
                result[order_ref[p], rows, :] = total[p * planes : (p + 1) * planes]

    in_steps(grid_edge // 2 // group, last_rows, last_lanes, last_store)

    if last:
        for k in range(slots):
            terms = result[k]
            if has_prior:
                terms += prior_ref[k]
            outs[k % 2][k // 2] = terms
    elif has_prior:
        result[...] += prior_ref[...]


def pair_terms(order, home, other, kernel, prior, last):
    grid_edge, plane_size = home.shape
    slots = order.shape[0]
    basis = real_basis(grid_edge)
    mixed = np.concatenate([np.arange(0, grid_edge, 2), np.arange(1, grid_edge, 2)])
    tables = (
        left_table(basis),
        left_table(basis[:, mixed]),
        left_table(basis.T[mixed]),
        left_table(basis.T),
        right_table(basis.T, grid_edge, half),
        right_table(basis, half, grid_edge),
    )
    slot_rows = grid_edge // slots * plane_size // lanes
    pitch = -(-grid_edge // 8) * 8 + 4
    whole = jax.ShapeDtypeStruct((slots, slot_rows, lanes), jnp.float32)
    part = jax.ShapeDtypeStruct((slots // 2, slot_rows, lanes), jnp.float32)
    vmem = pl.BlockSpec(memory_space=pltpu.VMEM)
    operands = [order, home, other, kernel, *(jnp.asarray(t) for t in tables)]
    operands += [] if prior is None else [prior]
    scratch = [pltpu.VMEM((grid_edge // 2 * pitch, lanes), jnp.float32)] * 2
    scratch += [pltpu.VMEM(whole.shape, jnp.float32)] if last else []
    return pl.pallas_call(
        functools.partial(pair_kernel, grid_edge, slots, prior is not None, last),
        out_shape=(part, part) if last else whole,
        in_specs=[pl.BlockSpec(memory_space=pltpu.SMEM)] + [vmem] * (len(operands) - 1),
        out_specs=(vmem, vmem) if last else vmem,
        scratch_shapes=scratch,
        compiler_params=pltpu.CompilerParams(vmem_limit_bytes=32 * 1024 * 1024),
        cost_estimate=pl.CostEstimate(flops=10**9, bytes_accessed=2 * 10**6, transcendentals=0),
    )(*operands)


def fetch(block, cycle_size, groups):
    across = groups + groups // 2
    routes = ([], [])
    for source in range(cycle_size):
        inner = 4 * source // cycle_size in (1, 2)
        for g in range(groups):
            near = sum(groups >> bit + 1 for bit in range(groups.bit_length() - 1) if g >> bit & 1)
            for turn, mask in enumerate((near ^ across, near) if inner else (near, near ^ across)):
                routes[turn].append((source * groups + g, (source ^ mask) * groups + g))
    first = lax.ppermute(block, ("blk", "off"), routes[0])
    second = lax.ppermute(block, ("blk", "off"), routes[1])
    return first, second


def scattered_sum(near, far, groups):
    bit = 1
    while True:
        arrived = lax.ppermute(far, "off", [(g, g ^ bit) for g in range(groups)])
        near = near + arrived
        bit *= 2
        if bit == groups:
            return near[0]
        near, far = near[0::2], near[1::2]


def on_device(orbitals):
    band_count, grid_edge, plane_size = orbitals.shape
    cycle_size, groups = lax.axis_size("blk"), lax.axis_size("off")
    if cycle_size != 2 * groups or groups & (groups - 1) or groups < 2 or grid_edge > half:
        raise ValueError("unsupported mesh")
    me = lax.axis_index("off")
    first, second = fetch(orbitals, cycle_size, groups)
    kernel = screened_kernel(grid_edge)
    order = jnp.arange(groups, dtype=jnp.int32) ^ me
    rows = []
    for home in orbitals:
        others = [*first, *second]
        terms = None
        for other in others[:-1]:
            terms = pair_terms(order, home, other, kernel, terms, False)
        near, far = pair_terms(order, home, others[-1], kernel, terms, True)
        rows.append(scattered_sum(near, far, groups))
    return jnp.stack(rows).reshape(band_count, grid_edge // groups, plane_size)


def solution(mesh):
    return jax.shard_map(
        on_device,
        mesh=mesh,
        in_specs=(P("blk", None, None),),
        out_specs=P("blk", "off", None),
        check_vma=False,
    )
```

```python
import functools
import math

import jax
import jax.numpy as jnp
import numpy as np
from jax import lax
from jax.experimental import pallas as pl
from jax.experimental.pallas import tpu as pltpu
from jax.sharding import PartitionSpec as P


cell_edge = 59.0
screen_rate = 0.106
lanes = 128
half = lanes // 2


def signed_points(grid_edge):
    points = np.arange(grid_edge)
    return np.where(points > grid_edge // 2, points - grid_edge, points)


def real_basis(grid_edge):
    points = np.arange(grid_edge)
    angles = 2.0 * np.pi / grid_edge * (points[:, None] * points[None, :] % grid_edge)
    rows = np.where(points[:, None] <= grid_edge // 2, np.cos(angles), np.sin(angles))
    single = (points == 0) | (2 * points == grid_edge)
    return rows * np.sqrt(np.where(single, 1.0, 2.0) / grid_edge)[:, None]


def in_two(values):
    high = values.astype(jnp.bfloat16)
    low = (values - high.astype(np.float64)).astype(jnp.bfloat16)
    return high, low


def left_table(matrix):
    high, low = in_two(matrix)
    return np.concatenate([high, high, low], axis=1)


def right_table(matrix):
    edge = matrix.shape[0]
    both = np.zeros((lanes, lanes))
    both[:edge, :edge] = matrix
    both[half : half + edge, half : half + edge] = matrix
    high, low = in_two(both)
    return np.block([[high, low], [high, np.zeros_like(low)]])


def screened_kernel(grid_edge):
    signed = signed_points(grid_edge)
    row = np.zeros(lanes, np.int32)
    row[:grid_edge] = signed**2
    row[half : half + grid_edge] = signed**2
    squares = jnp.asarray(signed**2, jnp.int32)
    squared = squares[:, None, None] + squares[None, :, None] + jnp.asarray(row)[None, None, :]
    wave_sq = squared.astype(jnp.float32) * jnp.float32((2.0 * math.pi / cell_edge) ** 2)
    safe_sq = jnp.where(squared == 0, jnp.float32(1.0), wave_sq)
    screened = 4.0 * math.pi * -jnp.expm1(-safe_sq / (4.0 * screen_rate**2)) / safe_sq
    return jnp.where(squared == 0, jnp.float32(math.pi / screen_rate**2), screened)


def split(values):
    high = values.astype(jnp.bfloat16)
    low = (values - high.astype(jnp.float32)).astype(jnp.bfloat16)
    return high, low


def dot(left, right):
    return jnp.dot(left, right, preferred_element_type=jnp.float32)


def rows_products(table, slabs):
    done = []
    for first in range(0, len(slabs), 2):
        columns = []
        for slab in slabs[first : first + 2]:
            high, low = split(slab)
            columns.append(jnp.concatenate([high, low, high], axis=0))
        product = dot(table, jnp.concatenate(columns, axis=1))
        done += [product[:, k * lanes : (k + 1) * lanes] for k in range(len(columns))]
    return done


def lanes_product(slabs, table):
    high, low = split(jnp.concatenate(slabs, axis=0))
    return dot(jnp.concatenate([high, low], axis=1), table)


def lanes_result(product, count):
    edge = product.shape[0] // count
    product = product[:, :lanes] + product[:, lanes:]
    return [product[k * edge : (k + 1) * edge] for k in range(count)]


def in_steps(count, *steps):
    held = [{} for _ in steps]
    for time in range(count + len(steps) - 1):
        for n, step in enumerate(steps):
            item = time - n
            if 0 <= item < count:
                given = (held[n - 1].pop(item),) if n else ()
                held[n][item] = step(item, *given)


def pair_kernel(
    grid_edge, slots, order_ref, home_ref, ahead_ref, behind_ref, kernel_ref,
    left_fwd_ref, left_back_ref, right_fwd_ref, right_back_ref, near_ref, far_ref, work, back, result,
):
    group = lanes // math.gcd(lanes, grid_edge)
    blocks = grid_edge // group
    tiles = group * grid_edge // lanes
    pitch = work.shape[0] // grid_edge
    planes = grid_edge // slots
    row_tiles = grid_edge * grid_edge // lanes
    lane = lax.broadcasted_iota(jnp.int32, (grid_edge, lanes), 1)
    shifted = (lane + half) % lanes

    def tiles_of(ref, block):
        first = block * tiles
        return [
            ref[:, (first + t) * lanes : (first + t + 1) * lanes].astype(jnp.float32)
            for t in range(tiles)
        ]

    def turn(values, amount):
        amount %= lanes
        return pltpu.roll(values, amount, 1) if amount else values

    def first_lanes(block):
        home = tiles_of(home_ref, block)
        first = [a * b for a, b in zip(home, tiles_of(ahead_ref, block))]
        second = [turn(a * b, half) for a, b in zip(home, tiles_of(behind_ref, block))]
        slabs = []
        for k in range(group):
            tile, offset = divmod(k * grid_edge, lanes)
            in_first = ((lane + (lanes - offset)) % lanes) < half
            this_a, this_b = first[tile], second[tile]
            if offset + grid_edge > lanes:
                this_a = jnp.where(lane >= offset, this_a, first[tile + 1])
                this_b = jnp.where(shifted >= offset, this_b, second[tile + 1])
            slabs.append(turn(jnp.where(in_first, this_a, this_b), -offset))
        return lanes_product(slabs, right_fwd_ref[...])

    def first_rows(block, product):
        return rows_products(left_fwd_ref[...], lanes_result(product, group))

    def first_store(block, slabs):
        for k, slab in enumerate(slabs):
            work[pl.ds((block * group + k) * pitch, grid_edge), :] = slab

    in_steps(blocks, first_lanes, first_rows, first_store)

    together = 2

    def rows_of(block):
        return [pl.ds(block * together + k, grid_edge, stride=pitch) for k in range(together)]

    def middle_forward(block):
        return rows_products(left_fwd_ref[...], [work[r, :] for r in rows_of(block)])

    def middle_back(block, slabs):
        slabs = [slab * kernel_ref[block * together + k] for k, slab in enumerate(slabs)]
        return rows_products(left_back_ref[...], slabs)

    def middle_store(block, slabs):
        for r, slab in zip(rows_of(block), slabs):
            back[r, :] = slab

    in_steps(grid_edge // together, middle_forward, middle_back, middle_store)

    def last_rows(block):
        slabs = [back[pl.ds((block * group + k) * pitch, grid_edge), :] for k in range(group)]
        return rows_products(left_back_ref[...], slabs)

    def last_lanes(block, slabs):
        return lanes_product(slabs, right_back_ref[...])

    def last_store(block, product):
        slabs = [turn(slab, k * grid_edge) for k, slab in enumerate(lanes_result(product, group))]
        ahead = tiles_of(ahead_ref, block)
        behind = tiles_of(behind_ref, block)
        for t in range(tiles):
            sources = range(t * lanes // grid_edge, ((t + 1) * lanes - 1) // grid_edge + 1)
            dense_a = dense_b = slabs[sources[0]]
            for k in sources[1:]:
                edge_lane = k * grid_edge - t * lanes
                dense_a = jnp.where(lane >= edge_lane, slabs[k], dense_a)
                dense_b = jnp.where(shifted >= edge_lane, slabs[k], dense_b)
            total = -0.25 * (dense_a * ahead[t] + turn(dense_b, half) * behind[t])
            rows = pl.ds(block * tiles + t, planes, stride=row_tiles)
            for p in range(slots):
                result[order_ref[p], rows, :] = total[p * planes : (p + 1) * planes]

    in_steps(blocks, last_rows, last_lanes, last_store)

    for k in range(slots // 2):
        near_ref[k] = result[2 * k]
        far_ref[k] = result[2 * k + 1]


def pair_terms(order, home, ahead, behind, kernel):
    grid_edge, plane_size = home.shape
    slots = order.shape[0]
    basis = real_basis(grid_edge)
    tables = (left_table(basis), left_table(basis.T), right_table(basis.T), right_table(basis))
    slot_rows = grid_edge // slots * plane_size // lanes
    pitch = -(-grid_edge // 8) * 8 + 4
    part = jax.ShapeDtypeStruct((slots // 2, slot_rows, lanes), jnp.float32)
    vmem = pl.BlockSpec(memory_space=pltpu.VMEM)
    return pl.pallas_call(
        functools.partial(pair_kernel, grid_edge, slots),
        out_shape=(part, part),
        in_specs=[pl.BlockSpec(memory_space=pltpu.SMEM)] + [vmem] * 8,
        out_specs=(vmem, vmem),
        scratch_shapes=[
            pltpu.VMEM((grid_edge * pitch, lanes), jnp.float32),
            pltpu.VMEM((grid_edge * pitch, lanes), jnp.float32),
            pltpu.VMEM((slots, slot_rows, lanes), jnp.float32),
        ],
        compiler_params=pltpu.CompilerParams(vmem_limit_bytes=32 * 1024 * 1024),
        cost_estimate=pl.CostEstimate(flops=2 * 10**9, bytes_accessed=3 * 10**6, transcendentals=0),
    )(order, home, ahead, behind, kernel, *(jnp.asarray(t) for t in tables))


def fetch(block, cycle_size, groups):
    routes = ([], [])
    for source in range(cycle_size):
        for g in range(groups):
            near = sum(groups >> bit + 1 for bit in range(groups.bit_length() - 1) if g >> bit & 1)
            for route, mask in zip(routes, (near, near ^ (groups + 1))):
                route.append((source * groups + g, (source ^ mask) * groups + g))
    near = lax.ppermute(block, ("blk", "off"), routes[0])
    across = lax.ppermute(block, ("blk", "off"), routes[1])
    return near, across


def scattered_sum(near, far, groups):
    bit = 1
    while True:
        arrived = lax.ppermute(far, "off", [(g, g ^ bit) for g in range(groups)])
        near = near + arrived
        bit *= 2
        if bit == groups:
            return near[0]
        near, far = near[0::2], near[1::2]


def on_device(orbitals):
    band_count, grid_edge, plane_size = orbitals.shape
    cycle_size, groups = lax.axis_size("blk"), lax.axis_size("off")
    if cycle_size != 2 * groups or groups & (groups - 1) or groups < 2 or grid_edge > half:
        raise ValueError("unsupported mesh")
    me = lax.axis_index("off")
    near, across = fetch(orbitals, cycle_size, groups)
    kernel = screened_kernel(grid_edge)
    order = jnp.arange(groups, dtype=jnp.int32) ^ me
    rows = []
    for i in range(band_count):
        own = rest = 0.0
        for j in range(band_count):
            terms = pair_terms(order, orbitals[i], near[j], across[j], kernel)
            own, rest = own + terms[0], rest + terms[1]
        rows.append(scattered_sum(own, rest, groups))
    return jnp.stack(rows).reshape(band_count, grid_edge // groups, plane_size)


def solution(mesh):
    return jax.shard_map(
        on_device,
        mesh=mesh,
        in_specs=(P("blk", None, None),),
        out_specs=P("blk", "off", None),
        check_vma=False,
    )
```

```python
import functools
import math

import jax
import jax.numpy as jnp
import numpy as np
from jax import lax
from jax.experimental import pallas as pl
from jax.experimental.pallas import tpu as pltpu
from jax.sharding import PartitionSpec as P


cell_edge = 59.0
screen_rate = 0.106
lanes = 128
half = lanes // 2


def signed_points(grid_edge):
    points = np.arange(grid_edge)
    return np.where(points > grid_edge // 2, points - grid_edge, points)


def real_basis(grid_edge):
    points = np.arange(grid_edge)
    angles = 2.0 * np.pi / grid_edge * (points[:, None] * points[None, :] % grid_edge)
    rows = np.where(points[:, None] <= grid_edge // 2, np.cos(angles), np.sin(angles))
    single = (points == 0) | (2 * points == grid_edge)
    return rows * np.sqrt(np.where(single, 1.0, 2.0) / grid_edge)[:, None]


def in_two(values):
    high = values.astype(jnp.bfloat16)
    low = (values - high.astype(np.float64)).astype(jnp.bfloat16)
    return high, low


def left_table(matrix):
    high, low = in_two(matrix)
    return np.concatenate([high, high, low], axis=1)


def right_table(matrix, start_in, start_out):
    edge = matrix.shape[0]
    both = np.zeros((lanes, lanes))
    both[:edge, :edge] = matrix
    both[start_in : start_in + edge, start_out : start_out + edge] = matrix
    high, low = in_two(both)
    return np.block([[high, low], [high, np.zeros_like(low)]])


def screened_kernel(grid_edge):
    signed = signed_points(grid_edge)
    row = np.zeros(lanes, np.int32)
    row[:grid_edge] = signed**2
    row[half : half + grid_edge] = signed**2
    pair = np.where(np.arange(lanes) < half, signed[0::2, None] ** 2, signed[1::2, None] ** 2) + row
    squared = jnp.asarray(pair, jnp.int32)[:, None, :] + jnp.asarray(signed**2, jnp.int32)[None, :, None]
    wave_sq = squared.astype(jnp.float32) * jnp.float32((2.0 * math.pi / cell_edge) ** 2)
    safe_sq = jnp.where(squared == 0, jnp.float32(1.0), wave_sq)
    screened = 4.0 * math.pi * -jnp.expm1(-safe_sq / (4.0 * screen_rate**2)) / safe_sq
    return jnp.where(squared == 0, jnp.float32(math.pi / screen_rate**2), screened)


def split(values):
    high = values.astype(jnp.bfloat16)
    low = (values - high.astype(jnp.float32)).astype(jnp.bfloat16)
    return high, low


def dot(left, right):
    return jnp.dot(left, right, preferred_element_type=jnp.float32)


def rows_products(table, slabs):
    done = []
    for first in range(0, len(slabs), 2):
        columns = []
        for slab in slabs[first : first + 2]:
            high, low = split(slab)
            columns.append(jnp.concatenate([high, low, high], axis=0))
        product = dot(table, jnp.concatenate(columns, axis=1))
        done += [product[:, k * lanes : (k + 1) * lanes] for k in range(len(columns))]
    return done


def lanes_product(slabs, table):
    high, low = split(jnp.concatenate(slabs, axis=0))
    return dot(jnp.concatenate([high, low], axis=1), table)


def lanes_result(product, count):
    edge = product.shape[0] // count
    product = product[:, :lanes] + product[:, lanes:]
    return [product[k * edge : (k + 1) * edge] for k in range(count)]


def in_steps(count, *steps):
    held = [{} for _ in steps]
    for time in range(count + len(steps) - 1):
        for n, step in enumerate(steps):
            item = time - n
            if 0 <= item < count:
                given = (held[n - 1].pop(item),) if n else ()
                held[n][item] = step(item, *given)


def pair_kernel(grid_edge, slots, has_prior, last, *refs):
    refs = list(refs)
    order_ref, home_ref, other_ref, kernel_ref = refs[:4]
    left_first_ref, left_fwd_ref, left_back_ref, left_last_ref, right_fwd_ref, right_back_ref = refs[4:10]
    prior_ref = refs[10] if has_prior else None
    outs = refs[10 + has_prior : -2 - last]
    work, back = refs[-2 - last], refs[-1 - last]
    result = refs[-1] if last else outs[0]

    line = 2 * grid_edge
    group = lanes // math.gcd(lanes, line)
    tiles = group * line // lanes
    pitch = work.shape[0] // (grid_edge // 2)
    planes = grid_edge // slots
    row_tiles = grid_edge * grid_edge // lanes
    lane = lax.broadcasted_iota(jnp.int32, (grid_edge, lanes), 1)
    together = 2 if grid_edge % 4 == 0 else 1
    in_first = lax.broadcasted_iota(jnp.int32, (grid_edge // 2, lanes), 1) < half

    def tiles_of(ref, block):
        first = block * tiles
        return [
            ref[:, (first + t) * lanes : (first + t + 1) * lanes].astype(jnp.float32)
            for t in range(tiles)
        ]

    def turn(values, amount):
        amount %= lanes
        return pltpu.roll(values, amount, 1) if amount else values

    def first_lanes(block):
        dense = [a * b for a, b in zip(tiles_of(home_ref, block), tiles_of(other_ref, block))]
        slabs = []
        for k in range(group):
            tile, offset = divmod(k * line, lanes)
            slab = dense[tile]
            if offset + line > lanes:
                slab = jnp.where(lane >= offset, slab, dense[tile + 1])
            slabs.append(turn(slab, -offset))
        return lanes_product(slabs, right_fwd_ref[...])

    def first_rows(block, product):
        return rows_products(left_first_ref[...], lanes_result(product, group))

    def first_store(block, slabs):
        for k, slab in enumerate(slabs):
            work[pl.ds((block * group + k) * pitch, grid_edge), :] = slab

    in_steps(grid_edge // 2 // group, first_lanes, first_rows, first_store)

    def rows_of(block):
        start = 2 * block * together
        return [
            [pl.ds(start + 2 * k + d, grid_edge // 2, stride=pitch) for d in range(2)]
            for k in range(together)
        ]

    def middle_forward(block):
        slabs = []
        for pair in rows_of(block):
            even, odd = (work[r, :] for r in pair)
            top = jnp.where(in_first, even, turn(odd, half))
            bottom = jnp.where(in_first, turn(even, half), odd)
            slabs.append(jnp.concatenate([top, bottom], axis=0))
        return rows_products(left_fwd_ref[...], slabs)

    def middle_back(block, slabs):
        slabs = [slab * kernel_ref[block * together + k] for k, slab in enumerate(slabs)]
        return rows_products(left_back_ref[...], slabs)

    def middle_store(block, slabs):
        for (row_even, row_odd), slab in zip(rows_of(block), slabs):
            top, bottom = slab[: grid_edge // 2], slab[grid_edge // 2 :]
            back[row_even, :] = jnp.where(in_first, top, turn(bottom, half))
            back[row_odd, :] = jnp.where(in_first, turn(top, half), bottom)

    in_steps(grid_edge // 2 // together, middle_forward, middle_back, middle_store)

    def last_rows(block):
        slabs = [back[pl.ds((block * group + k) * pitch, grid_edge), :] for k in range(group)]
        return rows_products(left_last_ref[...], slabs)

    def last_lanes(block, slabs):
        return lanes_product(slabs, right_back_ref[...])

    def last_store(block, product):
        slabs = [turn(slab, k * line) for k, slab in enumerate(lanes_result(product, group))]
        other = tiles_of(other_ref, block)
        for t in range(tiles):
            sources = range(t * lanes // line, ((t + 1) * lanes - 1) // line + 1)
            dense = slabs[sources[0]]
            for k in sources[1:]:
                dense = jnp.where(lane >= k * line - t * lanes, slabs[k], dense)
            total = -0.25 * (dense * other[t])
            rows = pl.ds(block * tiles + t, planes, stride=row_tiles)
            for p in range(slots):
                result[order_ref[p], rows, :] = total[p * planes : (p + 1) * planes]

    in_steps(grid_edge // 2 // group, last_rows, last_lanes, last_store)

    if last:
        for k in range(slots):
            terms = result[k]
            if has_prior:
                terms += prior_ref[k]
            outs[k % 2][k // 2] = terms
    elif has_prior:
        result[...] += prior_ref[...]


def pair_terms(order, home, other, kernel, prior, last):
    grid_edge, plane_size = home.shape
    slots = order.shape[0]
    basis = real_basis(grid_edge)
    mixed = np.concatenate([np.arange(0, grid_edge, 2), np.arange(1, grid_edge, 2)])
    tables = (
        left_table(basis),
        left_table(basis[:, mixed]),
        left_table(basis.T[mixed]),
        left_table(basis.T),
        right_table(basis.T, grid_edge, half),
        right_table(basis, half, grid_edge),
    )
    slot_rows = grid_edge // slots * plane_size // lanes
    pitch = -(-grid_edge // 8) * 8 + 4
    whole = jax.ShapeDtypeStruct((slots, slot_rows, lanes), jnp.float32)
    part = jax.ShapeDtypeStruct((slots // 2, slot_rows, lanes), jnp.float32)
    vmem = pl.BlockSpec(memory_space=pltpu.VMEM)
    operands = [order, home, other, kernel, *(jnp.asarray(t) for t in tables)]
    operands += [] if prior is None else [prior]
    scratch = [pltpu.VMEM((grid_edge // 2 * pitch, lanes), jnp.float32)] * 2
    scratch += [pltpu.VMEM(whole.shape, jnp.float32)] if last else []
    return pl.pallas_call(
        functools.partial(pair_kernel, grid_edge, slots, prior is not None, last),
        out_shape=(part, part) if last else whole,
        in_specs=[pl.BlockSpec(memory_space=pltpu.SMEM)] + [vmem] * (len(operands) - 1),
        out_specs=(vmem, vmem) if last else vmem,
        scratch_shapes=scratch,
        compiler_params=pltpu.CompilerParams(vmem_limit_bytes=32 * 1024 * 1024),
        cost_estimate=pl.CostEstimate(flops=10**9, bytes_accessed=2 * 10**6, transcendentals=0),
    )(*operands)


def fetch(block, cycle_size, groups):
    routes = ([], [])
    for source in range(cycle_size):
        for g in range(groups):
            for route, mask in zip(routes, (g // 2, g // 2 + groups // 2)):
                mask = cycle_size - 1 - (mask ^ groups // 2) if g % 2 else mask
                route.append((source * groups + g, (source ^ mask) * groups + g))
    first = lax.ppermute(block, ("blk", "off"), routes[0])
    second = lax.ppermute(block, ("blk", "off"), routes[1])
    return first, second


def scattered_sum(near, far, groups):
    bit = 1
    while True:
        arrived = lax.ppermute(far, "off", [(g, g ^ bit) for g in range(groups)])
        near = near + arrived
        bit *= 2
        if bit == groups:
            return near[0]
        near, far = near[0::2], near[1::2]


def on_device(orbitals):
    band_count, grid_edge, plane_size = orbitals.shape
    cycle_size, groups = lax.axis_size("blk"), lax.axis_size("off")
    if cycle_size != 2 * groups or groups & (groups - 1) or groups < 2 or grid_edge > half:
        raise ValueError("unsupported mesh")
    me = lax.axis_index("off")
    first, second = fetch(orbitals, cycle_size, groups)
    kernel = screened_kernel(grid_edge)
    order = jnp.arange(groups, dtype=jnp.int32) ^ me
    rows = []
    for home in orbitals:
        others = [*first, *second]
        terms = None
        for other in others[:-1]:
            terms = pair_terms(order, home, other, kernel, terms, False)
        own, rest = pair_terms(order, home, others[-1], kernel, terms, True)
        rows.append(scattered_sum(own, rest, groups))
    return jnp.stack(rows).reshape(band_count, grid_edge // groups, plane_size)


def solution(mesh):
    return jax.shard_map(
        on_device,
        mesh=mesh,
        in_specs=(P("blk", None, None),),
        out_specs=P("blk", "off", None),
        check_vma=False,
    )
```

```python
import functools
import math

import jax
import jax.numpy as jnp
import numpy as np
from jax import lax
from jax.experimental import pallas as pl
from jax.experimental.pallas import tpu as pltpu
from jax.sharding import PartitionSpec as P


cell_edge = 59.0
screen_rate = 0.106
lanes = 128
half = lanes // 2


def signed_points(grid_edge):
    points = np.arange(grid_edge)
    return np.where(points > grid_edge // 2, points - grid_edge, points)


def real_basis(grid_edge):
    points = np.arange(grid_edge)
    angles = 2.0 * np.pi / grid_edge * (points[:, None] * points[None, :] % grid_edge)
    rows = np.where(points[:, None] <= grid_edge // 2, np.cos(angles), np.sin(angles))
    single = (points == 0) | (2 * points == grid_edge)
    return rows * np.sqrt(np.where(single, 1.0, 2.0) / grid_edge)[:, None]


def in_two(values):
    high = values.astype(jnp.bfloat16)
    low = (values - high.astype(np.float64)).astype(jnp.bfloat16)
    return high, low


def left_table(matrix):
    high, low = in_two(matrix)
    return np.concatenate([high, high, low], axis=1)


def right_table(matrix, start_in, start_out):
    edge = matrix.shape[0]
    both = np.zeros((lanes, lanes))
    both[:edge, :edge] = matrix
    both[start_in : start_in + edge, start_out : start_out + edge] = matrix
    high, low = in_two(both)
    return np.block([[high, low], [high, np.zeros_like(low)]])


def screened_kernel(grid_edge):
    signed = signed_points(grid_edge)
    row = np.zeros(lanes, np.int32)
    row[:grid_edge] = signed**2
    row[half : half + grid_edge] = signed**2
    pair = np.where(np.arange(lanes) < half, signed[0::2, None] ** 2, signed[1::2, None] ** 2) + row
    squared = jnp.asarray(pair, jnp.int32)[:, None, :] + jnp.asarray(signed**2, jnp.int32)[None, :, None]
    wave_sq = squared.astype(jnp.float32) * jnp.float32((2.0 * math.pi / cell_edge) ** 2)
    safe_sq = jnp.where(squared == 0, jnp.float32(1.0), wave_sq)
    screened = 4.0 * math.pi * -jnp.expm1(-safe_sq / (4.0 * screen_rate**2)) / safe_sq
    return jnp.where(squared == 0, jnp.float32(math.pi / screen_rate**2), screened)


def split(values):
    high = values.astype(jnp.bfloat16)
    low = (values - high.astype(jnp.float32)).astype(jnp.bfloat16)
    return high, low


def dot(left, right):
    return jnp.dot(left, right, preferred_element_type=jnp.float32)


def rows_products(table, slabs):
    done = []
    for first in range(0, len(slabs), 2):
        columns = []
        for slab in slabs[first : first + 2]:
            high, low = split(slab)
            columns.append(jnp.concatenate([high, low, high], axis=0))
        product = dot(table, jnp.concatenate(columns, axis=1))
        done += [product[:, k * lanes : (k + 1) * lanes] for k in range(len(columns))]
    return done


def lanes_product(slabs, table):
    high, low = split(jnp.concatenate(slabs, axis=0))
    return dot(jnp.concatenate([high, low], axis=1), table)


def lanes_result(product, count):
    edge = product.shape[0] // count
    product = product[:, :lanes] + product[:, lanes:]
    return [product[k * edge : (k + 1) * edge] for k in range(count)]


def in_steps(count, *steps):
    held = [{} for _ in steps]
    for time in range(count + len(steps) - 1):
        for n, step in enumerate(steps):
            item = time - n
            if 0 <= item < count:
                given = (held[n - 1].pop(item),) if n else ()
                held[n][item] = step(item, *given)


def pair_kernel(grid_edge, slots, has_prior, last, *refs):
    refs = list(refs)
    home_ref, other_ref, kernel_ref = refs[:3]
    left_first_ref, left_fwd_ref, left_back_ref, left_last_ref, right_fwd_ref, right_back_ref = refs[3:9]
    prior_ref = refs[9] if has_prior else None
    outs = refs[9 + has_prior : -2 - last]
    work, back = refs[-2 - last], refs[-1 - last]
    result = refs[-1] if last else outs[0]

    me = lax.axis_index("off")
    line = 2 * grid_edge
    group = lanes // math.gcd(lanes, line)
    tiles = group * line // lanes
    pitch = work.shape[0] // (grid_edge // 2)
    planes = grid_edge // slots
    row_tiles = grid_edge * grid_edge // lanes
    lane = lax.broadcasted_iota(jnp.int32, (grid_edge, lanes), 1)
    together = 2 if grid_edge % 4 == 0 else 1
    in_first = lax.broadcasted_iota(jnp.int32, (grid_edge // 2, lanes), 1) < half

    def tiles_of(ref, block):
        first = block * tiles
        return [
            ref[:, (first + t) * lanes : (first + t + 1) * lanes].astype(jnp.float32)
            for t in range(tiles)
        ]

    def turn(values, amount):
        amount %= lanes
        return pltpu.roll(values, amount, 1) if amount else values

    def first_lanes(block):
        dense = [a * b for a, b in zip(tiles_of(home_ref, block), tiles_of(other_ref, block))]
        slabs = []
        for k in range(group):
            tile, offset = divmod(k * line, lanes)
            slab = dense[tile]
            if offset + line > lanes:
                slab = jnp.where(lane >= offset, slab, dense[tile + 1])
            slabs.append(turn(slab, -offset))
        return lanes_product(slabs, right_fwd_ref[...])

    def first_rows(block, product):
        return rows_products(left_first_ref[...], lanes_result(product, group))

    def first_store(block, slabs):
        for k, slab in enumerate(slabs):
            work[pl.ds((block * group + k) * pitch, grid_edge), :] = slab

    in_steps(grid_edge // 2 // group, first_lanes, first_rows, first_store)

    def rows_of(block):
        start = 2 * block * together
        return [
            [pl.ds(start + 2 * k + d, grid_edge // 2, stride=pitch) for d in range(2)]
            for k in range(together)
        ]

    def middle_forward(block):
        slabs = []
        for pair in rows_of(block):
            even, odd = (work[r, :] for r in pair)
            top = jnp.where(in_first, even, turn(odd, half))
            bottom = jnp.where(in_first, turn(even, half), odd)
            slabs.append(jnp.concatenate([top, bottom], axis=0))
        return rows_products(left_fwd_ref[...], slabs)

    def middle_back(block, slabs):
        slabs = [slab * kernel_ref[block * together + k] for k, slab in enumerate(slabs)]
        return rows_products(left_back_ref[...], slabs)

    def middle_store(block, slabs):
        for (row_even, row_odd), slab in zip(rows_of(block), slabs):
            top, bottom = slab[: grid_edge // 2], slab[grid_edge // 2 :]
            back[row_even, :] = jnp.where(in_first, top, turn(bottom, half))
            back[row_odd, :] = jnp.where(in_first, turn(top, half), bottom)

    in_steps(grid_edge // 2 // together, middle_forward, middle_back, middle_store)

    def last_rows(block):
        slabs = [back[pl.ds((block * group + k) * pitch, grid_edge), :] for k in range(group)]
        return rows_products(left_last_ref[...], slabs)

    def last_lanes(block, slabs):
        return lanes_product(slabs, right_back_ref[...])

    def last_store(block, product):
        slabs = [turn(slab, k * line) for k, slab in enumerate(lanes_result(product, group))]
        other = tiles_of(other_ref, block)
        for t in range(tiles):
            sources = range(t * lanes // line, ((t + 1) * lanes - 1) // line + 1)
            dense = slabs[sources[0]]
            for k in sources[1:]:
                dense = jnp.where(lane >= k * line - t * lanes, slabs[k], dense)
            total = -0.25 * (dense * other[t])
            rows = pl.ds(block * tiles + t, planes, stride=row_tiles)
            for p in range(slots):
                result[me ^ p, rows, :] = total[p * planes : (p + 1) * planes]

    in_steps(grid_edge // 2 // group, last_rows, last_lanes, last_store)

    if last:
        for k in range(slots):
            terms = result[k]
            if has_prior:
                terms += prior_ref[k]
            outs[k % 2][k // 2] = terms
    elif has_prior:
        result[...] += prior_ref[...]


def pair_terms(slots, home, other, kernel, prior, last):
    grid_edge, plane_size = home.shape
    basis = real_basis(grid_edge)
    mixed = np.concatenate([np.arange(0, grid_edge, 2), np.arange(1, grid_edge, 2)])
    tables = (
        left_table(basis),
        left_table(basis[:, mixed]),
        left_table(basis.T[mixed]),
        left_table(basis.T),
        right_table(basis.T, grid_edge, half),
        right_table(basis, half, grid_edge),
    )
    slot_rows = grid_edge // slots * plane_size // lanes
    pitch = -(-grid_edge // 8) * 8 + 4
    whole = jax.ShapeDtypeStruct((slots, slot_rows, lanes), jnp.float32)
    part = jax.ShapeDtypeStruct((slots // 2, slot_rows, lanes), jnp.float32)
    vmem = pl.BlockSpec(memory_space=pltpu.VMEM)
    operands = [home, other, kernel, *(jnp.asarray(t) for t in tables)]
    operands += [] if prior is None else [prior]
    scratch = [pltpu.VMEM((grid_edge // 2 * pitch, lanes), jnp.float32)] * 2
    scratch += [pltpu.VMEM(whole.shape, jnp.float32)] if last else []
    return pl.pallas_call(
        functools.partial(pair_kernel, grid_edge, slots, prior is not None, last),
        out_shape=(part, part) if last else whole,
        in_specs=[vmem] * len(operands),
        out_specs=(vmem, vmem) if last else vmem,
        scratch_shapes=scratch,
        compiler_params=pltpu.CompilerParams(vmem_limit_bytes=32 * 1024 * 1024),
        cost_estimate=pl.CostEstimate(flops=10**9, bytes_accessed=2 * 10**6, transcendentals=0),
    )(*operands)


def fetch(block, cycle_size, groups):
    routes = ([], [])
    for source in range(cycle_size):
        for g in range(groups):
            for route, mask in zip(routes, (g // 2, g // 2 + groups // 2)):
                mask = cycle_size - 1 - (mask ^ groups // 2) if g % 2 else mask
                route.append((source * groups + g, (source ^ mask) * groups + g))
    first = lax.ppermute(block, ("blk", "off"), routes[0])
    second = lax.ppermute(block, ("blk", "off"), routes[1])
    return first, second


def scattered_sum(near, far, groups):
    bit = 1
    while True:
        arrived = lax.ppermute(far, "off", [(g, g ^ bit) for g in range(groups)])
        near = near + arrived
        bit *= 2
        if bit == groups:
            return near[0]
        near, far = near[0::2], near[1::2]


def on_device(orbitals):
    band_count, grid_edge, plane_size = orbitals.shape
    cycle_size, groups = lax.axis_size("blk"), lax.axis_size("off")
    if cycle_size != 2 * groups or groups & (groups - 1) or groups < 2 or grid_edge > half:
        raise ValueError("unsupported mesh")
    first, second = fetch(orbitals, cycle_size, groups)
    kernel = screened_kernel(grid_edge)
    rows = []
    for home in orbitals:
        others = [*first, *second]
        terms = None
        for other in others[:-1]:
            terms = pair_terms(groups, home, other, kernel, terms, False)
        own, rest = pair_terms(groups, home, others[-1], kernel, terms, True)
        rows.append(scattered_sum(own, rest, groups))
    return jnp.stack(rows).reshape(band_count, grid_edge // groups, plane_size)


def solution(mesh):
    return jax.shard_map(
        on_device,
        mesh=mesh,
        in_specs=(P("blk", None, None),),
        out_specs=P("blk", "off", None),
        check_vma=False,
    )
```

```python
import functools
import math

import jax
import jax.numpy as jnp
import numpy as np
from jax import lax
from jax.experimental import pallas as pl
from jax.experimental.pallas import tpu as pltpu
from jax.sharding import PartitionSpec as P


cell_edge = 59.0
screen_rate = 0.106
lanes = 128
half = lanes // 2


def signed_points(grid_edge):
    points = np.arange(grid_edge)
    return np.where(points > grid_edge // 2, points - grid_edge, points)


def real_basis(grid_edge):
    points = np.arange(grid_edge)
    angles = 2.0 * np.pi / grid_edge * (points[:, None] * points[None, :] % grid_edge)
    rows = np.where(points[:, None] <= grid_edge // 2, np.cos(angles), np.sin(angles))
    single = (points == 0) | (2 * points == grid_edge)
    return rows * np.sqrt(np.where(single, 1.0, 2.0) / grid_edge)[:, None]


def in_two(values):
    high = values.astype(jnp.bfloat16)
    low = (values - high.astype(np.float64)).astype(jnp.bfloat16)
    return high, low


def left_table(matrix):
    high, low = in_two(matrix)
    return np.concatenate([high, high, low], axis=1)


def right_table(matrix, start_in, start_out):
    edge = matrix.shape[0]
    both = np.zeros((lanes, lanes))
    both[:edge, :edge] = matrix
    both[start_in : start_in + edge, start_out : start_out + edge] = matrix
    high, low = in_two(both)
    return np.block([[high, low], [high, np.zeros_like(low)]])


def screened_kernel(grid_edge):
    signed = signed_points(grid_edge)
    row = np.zeros(lanes, np.int32)
    row[:grid_edge] = signed**2
    row[half : half + grid_edge] = signed**2
    pair = np.where(np.arange(lanes) < half, signed[0::2, None] ** 2, signed[1::2, None] ** 2) + row
    squared = jnp.asarray(pair, jnp.int32)[:, None, :] + jnp.asarray(signed**2, jnp.int32)[None, :, None]
    wave_sq = squared.astype(jnp.float32) * jnp.float32((2.0 * math.pi / cell_edge) ** 2)
    safe_sq = jnp.where(squared == 0, jnp.float32(1.0), wave_sq)
    screened = 4.0 * math.pi * -jnp.expm1(-safe_sq / (4.0 * screen_rate**2)) / safe_sq
    return jnp.where(squared == 0, jnp.float32(math.pi / screen_rate**2), screened)


def split(values):
    high = values.astype(jnp.bfloat16)
    low = (values - high.astype(jnp.float32)).astype(jnp.bfloat16)
    return high, low


def dot(left, right):
    return jnp.dot(left, right, preferred_element_type=jnp.float32)


def rows_products(table, slabs):
    done = []
    for first in range(0, len(slabs), 2):
        columns = []
        for slab in slabs[first : first + 2]:
            high, low = split(slab)
            columns.append(jnp.concatenate([high, low, high], axis=0))
        product = dot(table, jnp.concatenate(columns, axis=1))
        done += [product[:, k * lanes : (k + 1) * lanes] for k in range(len(columns))]
    return done


def lanes_product(slabs, table):
    high, low = split(jnp.concatenate(slabs, axis=0))
    return dot(jnp.concatenate([high, low], axis=1), table)


def lanes_result(product, count):
    edge = product.shape[0] // count
    product = product[:, :lanes] + product[:, lanes:]
    return [product[k * edge : (k + 1) * edge] for k in range(count)]


def in_stages(count, *stages):
    results = [()] * count
    for stage in stages:
        results = [(stage(i, *given),) for i, given in enumerate(results)]


def pair_kernel(grid_edge, slots, has_prior, last, *refs):
    refs = list(refs)
    home_ref, other_ref, kernel_ref = refs[:3]
    left_first_ref, left_fwd_ref, left_back_ref, left_last_ref, right_fwd_ref, right_back_ref = refs[3:9]
    prior_ref = refs[9] if has_prior else None
    outs = refs[9 + has_prior : -2 - last]
    work, back = refs[-2 - last], refs[-1 - last]
    result = refs[-1] if last else outs[0]

    me = lax.axis_index("off")
    line = 2 * grid_edge
    group = lanes // math.gcd(lanes, line)
    tiles = group * line // lanes
    pitch = work.shape[0] // (grid_edge // 2)
    planes = grid_edge // slots
    row_tiles = grid_edge * grid_edge // lanes
    lane = lax.broadcasted_iota(jnp.int32, (grid_edge, lanes), 1)
    together = 2 if grid_edge % 4 == 0 else 1
    in_first = lax.broadcasted_iota(jnp.int32, (grid_edge // 2, lanes), 1) < half

    def tiles_of(ref, block):
        first = block * tiles
        return [
            ref[:, (first + t) * lanes : (first + t + 1) * lanes].astype(jnp.float32)
            for t in range(tiles)
        ]

    def turn(values, amount):
        amount %= lanes
        return pltpu.roll(values, amount, 1) if amount else values

    def first_lanes(block):
        dense = [a * b for a, b in zip(tiles_of(home_ref, block), tiles_of(other_ref, block))]
        slabs = []
        for k in range(group):
            tile, offset = divmod(k * line, lanes)
            slab = dense[tile]
            if offset + line > lanes:
                slab = jnp.where(lane >= offset, slab, dense[tile + 1])
            slabs.append(turn(slab, -offset))
        return lanes_product(slabs, right_fwd_ref[...])

    def first_rows(block, product):
        return rows_products(left_first_ref[...], lanes_result(product, group))

    def first_store(block, slabs):
        for k, slab in enumerate(slabs):
            work[pl.ds((block * group + k) * pitch, grid_edge), :] = slab

    in_stages(grid_edge // 2 // group, first_lanes, first_rows, first_store)

    def rows_of(block):
        start = 2 * block * together
        return [
            [pl.ds(start + 2 * k + d, grid_edge // 2, stride=pitch) for d in range(2)]
            for k in range(together)
        ]

    def middle_forward(block):
        slabs = []
        for pair in rows_of(block):
            even, odd = (work[r, :] for r in pair)
            top = jnp.where(in_first, even, turn(odd, half))
            bottom = jnp.where(in_first, turn(even, half), odd)
            slabs.append(jnp.concatenate([top, bottom], axis=0))
        return rows_products(left_fwd_ref[...], slabs)

    def middle_back(block, slabs):
        slabs = [slab * kernel_ref[block * together + k] for k, slab in enumerate(slabs)]
        return rows_products(left_back_ref[...], slabs)

    def middle_store(block, slabs):
        for (row_even, row_odd), slab in zip(rows_of(block), slabs):
            top, bottom = slab[: grid_edge // 2], slab[grid_edge // 2 :]
            back[row_even, :] = jnp.where(in_first, top, turn(bottom, half))
            back[row_odd, :] = jnp.where(in_first, turn(top, half), bottom)

    in_stages(grid_edge // 2 // together, middle_forward, middle_back, middle_store)

    def last_rows(block):
        slabs = [back[pl.ds((block * group + k) * pitch, grid_edge), :] for k in range(group)]
        return rows_products(left_last_ref[...], slabs)

    def last_lanes(block, slabs):
        return lanes_product(slabs, right_back_ref[...])

    def last_store(block, product):
        slabs = [turn(slab, k * line) for k, slab in enumerate(lanes_result(product, group))]
        other = tiles_of(other_ref, block)
        for t in range(tiles):
            sources = range(t * lanes // line, ((t + 1) * lanes - 1) // line + 1)
            dense = slabs[sources[0]]
            for k in sources[1:]:
                dense = jnp.where(lane >= k * line - t * lanes, slabs[k], dense)
            total = -0.25 * (dense * other[t])
            rows = pl.ds(block * tiles + t, planes, stride=row_tiles)
            for p in range(slots):
                result[me ^ p, rows, :] = total[p * planes : (p + 1) * planes]

    in_stages(grid_edge // 2 // group, last_rows, last_lanes, last_store)

    if last:
        for k in range(slots):
            terms = result[k]
            if has_prior:
                terms += prior_ref[k]
            outs[k % 2][k // 2] = terms
    elif has_prior:
        result[...] += prior_ref[...]


def pair_terms(slots, home, other, kernel, prior, last):
    grid_edge, plane_size = home.shape
    basis = real_basis(grid_edge)
    mixed = np.concatenate([np.arange(0, grid_edge, 2), np.arange(1, grid_edge, 2)])
    tables = (
        left_table(basis),
        left_table(basis[:, mixed]),
        left_table(basis.T[mixed]),
        left_table(basis.T),
        right_table(basis.T, grid_edge, half),
        right_table(basis, half, grid_edge),
    )
    slot_rows = grid_edge // slots * plane_size // lanes
    pitch = -(-grid_edge // 8) * 8 + 4
    whole = jax.ShapeDtypeStruct((slots, slot_rows, lanes), jnp.float32)
    part = jax.ShapeDtypeStruct((slots // 2, slot_rows, lanes), jnp.float32)
    vmem = pl.BlockSpec(memory_space=pltpu.VMEM)
    operands = [home, other, kernel, *(jnp.asarray(t) for t in tables)]
    operands += [] if prior is None else [prior]
    scratch = [pltpu.VMEM((grid_edge // 2 * pitch, lanes), jnp.float32)] * 2
    scratch += [pltpu.VMEM(whole.shape, jnp.float32)] if last else []
    return pl.pallas_call(
        functools.partial(pair_kernel, grid_edge, slots, prior is not None, last),
        out_shape=(part, part) if last else whole,
        in_specs=[vmem] * len(operands),
        out_specs=(vmem, vmem) if last else vmem,
        scratch_shapes=scratch,
        compiler_params=pltpu.CompilerParams(vmem_limit_bytes=32 * 1024 * 1024),
        cost_estimate=pl.CostEstimate(flops=10**9, bytes_accessed=2 * 10**6, transcendentals=0),
    )(*operands)


def fetch(block, cycle_size, groups):
    routes = ([], [])
    for source in range(cycle_size):
        for g in range(groups):
            for route, mask in zip(routes, (g // 2 + groups // 2, g // 2)):
                mask = cycle_size - 1 - mask if g % 2 else mask
                route.append((source * groups + g, (source ^ mask) * groups + g))
    first = lax.ppermute(block, ("blk", "off"), routes[0])
    second = lax.ppermute(block, ("blk", "off"), routes[1])
    return first, second


def scattered_sum(near, far, groups):
    bit = 1
    while True:
        arrived = lax.ppermute(far, "off", [(g, g ^ bit) for g in range(groups)])
        near = near + arrived
        bit *= 2
        if bit == groups:
            return near[0]
        near, far = near[0::2], near[1::2]


def on_device(orbitals):
    band_count, grid_edge, plane_size = orbitals.shape
    cycle_size, groups = lax.axis_size("blk"), lax.axis_size("off")
    if cycle_size != 2 * groups or groups & (groups - 1) or groups < 2 or grid_edge > half:
        raise ValueError("unsupported mesh")
    first, second = fetch(orbitals, cycle_size, groups)
    kernel = screened_kernel(grid_edge)
    rows = []
    for home in orbitals:
        others = [*first, *second]
        terms = None
        for other in others[:-1]:
            terms = pair_terms(groups, home, other, kernel, terms, False)
        own, rest = pair_terms(groups, home, others[-1], kernel, terms, True)
        rows.append(scattered_sum(own, rest, groups))
    return jnp.stack(rows).reshape(band_count, grid_edge // groups, plane_size)


def solution(mesh):
    return jax.shard_map(
        on_device,
        mesh=mesh,
        in_specs=(P("blk", None, None),),
        out_specs=P("blk", "off", None),
        check_vma=False,
    )
```

```python
import functools
import math

import jax
import jax.numpy as jnp
import numpy as np
from jax import lax
from jax.experimental import pallas as pl
from jax.experimental.pallas import tpu as pltpu
from jax.sharding import PartitionSpec as P


cell_edge = 59.0
screen_rate = 0.106
lanes = 128
half = lanes // 2


def signed_points(grid_edge):
    points = np.arange(grid_edge)
    return np.where(points > grid_edge // 2, points - grid_edge, points)


def real_basis(grid_edge):
    points = np.arange(grid_edge)
    angles = 2.0 * np.pi / grid_edge * (points[:, None] * points[None, :] % grid_edge)
    rows = np.where(points[:, None] <= grid_edge // 2, np.cos(angles), np.sin(angles))
    single = (points == 0) | (2 * points == grid_edge)
    return rows * np.sqrt(np.where(single, 1.0, 2.0) / grid_edge)[:, None]


def in_two(values):
    high = values.astype(jnp.bfloat16)
    low = (values - high.astype(np.float64)).astype(jnp.bfloat16)
    return high, low


def left_table(matrix):
    high, low = in_two(matrix)
    return np.concatenate([high, high, low], axis=1)


def right_table(matrix, start_in, start_out):
    edge = matrix.shape[0]
    both = np.zeros((lanes, lanes))
    both[:edge, :edge] = matrix
    both[start_in : start_in + edge, start_out : start_out + edge] = matrix
    high, low = in_two(both)
    return np.block([[high, low], [high, np.zeros_like(low)]])


def screened_kernel(grid_edge):
    signed = signed_points(grid_edge)
    row = np.zeros(lanes, np.int32)
    row[:grid_edge] = signed**2
    row[half : half + grid_edge] = signed**2
    pair = np.where(np.arange(lanes) < half, signed[0::2, None] ** 2, signed[1::2, None] ** 2) + row
    squared = jnp.asarray(pair, jnp.int32)[:, None, :] + jnp.asarray(signed**2, jnp.int32)[None, :, None]
    wave_sq = squared.astype(jnp.float32) * jnp.float32((2.0 * math.pi / cell_edge) ** 2)
    safe_sq = jnp.where(squared == 0, jnp.float32(1.0), wave_sq)
    screened = 4.0 * math.pi * -jnp.expm1(-safe_sq / (4.0 * screen_rate**2)) / safe_sq
    return jnp.where(squared == 0, jnp.float32(math.pi / screen_rate**2), screened)


def split(values):
    high = values.astype(jnp.bfloat16)
    low = (values - high.astype(jnp.float32)).astype(jnp.bfloat16)
    return high, low


def dot(left, right):
    return jnp.dot(left, right, preferred_element_type=jnp.float32)


def rows_products(table, slabs):
    done = []
    for first in range(0, len(slabs), 2):
        columns = []
        for slab in slabs[first : first + 2]:
            high, low = split(slab)
            columns.append(jnp.concatenate([high, low, high], axis=0))
        product = dot(table, jnp.concatenate(columns, axis=1))
        done += [product[:, k * lanes : (k + 1) * lanes] for k in range(len(columns))]
    return done


def lanes_product(slabs, table):
    high, low = split(jnp.concatenate(slabs, axis=0))
    return dot(jnp.concatenate([high, low], axis=1), table)


def lanes_result(product, count):
    edge = product.shape[0] // count
    product = product[:, :lanes] + product[:, lanes:]
    return [product[k * edge : (k + 1) * edge] for k in range(count)]


def in_stages(count, *stages):
    results = [()] * count
    for stage in stages:
        results = [(stage(i, *given),) for i, given in enumerate(results)]


def pair_kernel(grid_edge, slots, has_prior, last, *refs):
    refs = list(refs)
    home_ref, other_ref, kernel_ref = refs[:3]
    left_first_ref, left_fwd_ref, left_back_ref, left_last_ref, right_fwd_ref, right_back_ref = refs[3:9]
    prior_ref = refs[9] if has_prior else None
    outs = refs[9 + has_prior : -2 - last]
    work, back = refs[-2 - last], refs[-1 - last]
    result = refs[-1] if last else outs[0]

    me = lax.axis_index("off")
    line = 2 * grid_edge
    group = lanes // math.gcd(lanes, line)
    tiles = group * line // lanes
    pitch = work.shape[0] // (grid_edge // 2)
    planes = grid_edge // slots
    row_tiles = grid_edge * grid_edge // lanes
    lane = lax.broadcasted_iota(jnp.int32, (grid_edge, lanes), 1)
    together = 2 if grid_edge % 4 == 0 else 1
    in_first = lax.broadcasted_iota(jnp.int32, (grid_edge // 2, lanes), 1) < half

    def tiles_of(ref, block):
        first = block * tiles
        return [
            ref[:, (first + t) * lanes : (first + t + 1) * lanes].astype(jnp.float32)
            for t in range(tiles)
        ]

    def turn(values, amount):
        amount %= lanes
        return pltpu.roll(values, amount, 1) if amount else values

    def first_lanes(block):
        dense = [a * b for a, b in zip(tiles_of(home_ref, block), tiles_of(other_ref, block))]
        slabs = []
        for k in range(group):
            tile, offset = divmod(k * line, lanes)
            slab = dense[tile]
            if offset + line > lanes:
                slab = jnp.where(lane >= offset, slab, dense[tile + 1])
            slabs.append(turn(slab, -offset))
        return lanes_product(slabs, right_fwd_ref[...])

    def first_rows(block, product):
        return rows_products(left_first_ref[...], lanes_result(product, group))

    def first_store(block, slabs):
        for k, slab in enumerate(slabs):
            work[pl.ds((block * group + k) * pitch, grid_edge), :] = slab

    in_stages(grid_edge // 2 // group, first_lanes, first_rows, first_store)

    def rows_of(block):
        start = 2 * block * together
        return [
            [pl.ds(start + 2 * k + d, grid_edge // 2, stride=pitch) for d in range(2)]
            for k in range(together)
        ]

    def middle_forward(block):
        slabs = []
        for pair in rows_of(block):
            even, odd = (work[r, :] for r in pair)
            top = jnp.where(in_first, even, turn(odd, half))
            bottom = jnp.where(in_first, turn(even, half), odd)
            slabs.append(jnp.concatenate([top, bottom], axis=0))
        return rows_products(left_fwd_ref[...], slabs)

    def middle_back(block, slabs):
        slabs = [slab * kernel_ref[block * together + k] for k, slab in enumerate(slabs)]
        return rows_products(left_back_ref[...], slabs)

    def middle_store(block, slabs):
        for (row_even, row_odd), slab in zip(rows_of(block), slabs):
            top, bottom = slab[: grid_edge // 2], slab[grid_edge // 2 :]
            back[row_even, :] = jnp.where(in_first, top, turn(bottom, half))
            back[row_odd, :] = jnp.where(in_first, turn(top, half), bottom)

    in_stages(grid_edge // 2 // together, middle_forward, middle_back, middle_store)

    def last_rows(block):
        slabs = [back[pl.ds((block * group + k) * pitch, grid_edge), :] for k in range(group)]
        return rows_products(left_last_ref[...], slabs)

    def last_lanes(block, slabs):
        return lanes_product(slabs, right_back_ref[...])

    def last_store(block, product):
        slabs = [turn(slab, k * line) for k, slab in enumerate(lanes_result(product, group))]
        other = tiles_of(other_ref, block)
        for t in range(tiles):
            sources = range(t * lanes // line, ((t + 1) * lanes - 1) // line + 1)
            dense = slabs[sources[0]]
            for k in sources[1:]:
                dense = jnp.where(lane >= k * line - t * lanes, slabs[k], dense)
            total = -0.25 * (dense * other[t])
            rows = pl.ds(block * tiles + t, planes, stride=row_tiles)
            for p in range(slots):
                result[me ^ p, rows, :] = total[p * planes : (p + 1) * planes]

    in_stages(grid_edge // 2 // group, last_rows, last_lanes, last_store)

    if last:
        for k in range(slots):
            terms = result[k]
            if has_prior:
                terms += prior_ref[k]
            outs[k % 4][k // 4] = terms
    elif has_prior:
        result[...] += prior_ref[...]


def pair_terms(slots, home, other, kernel, prior, last):
    grid_edge, plane_size = home.shape
    basis = real_basis(grid_edge)
    mixed = np.concatenate([np.arange(0, grid_edge, 2), np.arange(1, grid_edge, 2)])
    tables = (
        left_table(basis),
        left_table(basis[:, mixed]),
        left_table(basis.T[mixed]),
        left_table(basis.T),
        right_table(basis.T, grid_edge, half),
        right_table(basis, half, grid_edge),
    )
    slot_rows = grid_edge // slots * plane_size // lanes
    pitch = -(-grid_edge // 8) * 8 + 4
    whole = jax.ShapeDtypeStruct((slots, slot_rows, lanes), jnp.float32)
    part = jax.ShapeDtypeStruct((slots // 4, slot_rows, lanes), jnp.float32)
    vmem = pl.BlockSpec(memory_space=pltpu.VMEM)
    operands = [home, other, kernel, *(jnp.asarray(t) for t in tables)]
    operands += [] if prior is None else [prior]
    scratch = [pltpu.VMEM((grid_edge // 2 * pitch, lanes), jnp.float32)] * 2
    scratch += [pltpu.VMEM(whole.shape, jnp.float32)] if last else []
    return pl.pallas_call(
        functools.partial(pair_kernel, grid_edge, slots, prior is not None, last),
        out_shape=(part,) * 4 if last else whole,
        in_specs=[vmem] * len(operands),
        out_specs=(vmem,) * 4 if last else vmem,
        scratch_shapes=scratch,
        compiler_params=pltpu.CompilerParams(vmem_limit_bytes=32 * 1024 * 1024),
        cost_estimate=pl.CostEstimate(flops=10**9, bytes_accessed=2 * 10**6, transcendentals=0),
    )(*operands)


def fetch(block, cycle_size, groups):
    routes = ([], [])
    for source in range(cycle_size):
        for g in range(groups):
            for route, mask in zip(routes, (groups - 1 - g // 2, g // 2)):
                mask = cycle_size - 1 - mask if g % 2 else mask
                route.append((source * groups + g, (source ^ mask) * groups + g))
    first = lax.ppermute(block, ("blk", "off"), routes[0])
    second = lax.ppermute(block, ("blk", "off"), routes[1])
    return first, second


def scattered_sum(parts, groups):
    to_neighbour = [(g, g ^ 1) for g in range(groups)]
    passed_on = lax.ppermute(parts[3], "off", to_neighbour)
    kept = lax.ppermute(parts[1], "off", to_neighbour)
    near, far = parts[0] + kept, parts[2] + passed_on
    bit = 2
    while True:
        arrived = lax.ppermute(far, "off", [(g, g ^ bit) for g in range(groups)])
        near = near + arrived
        bit *= 2
        if bit == groups:
            return near[0]
        near, far = near[0::2], near[1::2]


def on_device(orbitals):
    band_count, grid_edge, plane_size = orbitals.shape
    cycle_size, groups = lax.axis_size("blk"), lax.axis_size("off")
    if cycle_size != 2 * groups or groups & (groups - 1) or groups < 4 or grid_edge > half:
        raise ValueError("unsupported mesh")
    first, second = fetch(orbitals, cycle_size, groups)
    kernel = screened_kernel(grid_edge)
    rows = []
    for home in orbitals:
        others = [*first, *second]
        terms = None
        for other in others[:-1]:
            terms = pair_terms(groups, home, other, kernel, terms, False)
        parts = pair_terms(groups, home, others[-1], kernel, terms, True)
        rows.append(scattered_sum(parts, groups))
    return jnp.stack(rows).reshape(band_count, grid_edge // groups, plane_size)


def solution(mesh):
    return jax.shard_map(
        on_device,
        mesh=mesh,
        in_specs=(P("blk", None, None),),
        out_specs=P("blk", "off", None),
        check_vma=False,
    )
```

```python
import functools
import math

import jax
import jax.numpy as jnp
import numpy as np
from jax import lax
from jax.experimental import pallas as pl
from jax.experimental.pallas import tpu as pltpu
from jax.sharding import PartitionSpec as P


cell_edge = 59.0
screen_rate = 0.106
lanes = 128
half = lanes // 2


def signed_points(grid_edge):
    points = np.arange(grid_edge)
    return np.where(points > grid_edge // 2, points - grid_edge, points)


def real_basis(grid_edge):
    points = np.arange(grid_edge)
    angles = 2.0 * np.pi / grid_edge * (points[:, None] * points[None, :] % grid_edge)
    rows = np.where(points[:, None] <= grid_edge // 2, np.cos(angles), np.sin(angles))
    single = (points == 0) | (2 * points == grid_edge)
    return rows * np.sqrt(np.where(single, 1.0, 2.0) / grid_edge)[:, None]


def in_two(values):
    high = values.astype(jnp.bfloat16)
    low = (values - high.astype(np.float64)).astype(jnp.bfloat16)
    return high, low


def left_table(matrix):
    high, low = in_two(matrix)
    return np.concatenate([high, high, low], axis=1)


def right_table(matrix, start_in, start_out):
    edge = matrix.shape[0]
    both = np.zeros((lanes, lanes))
    both[:edge, :edge] = matrix
    both[start_in : start_in + edge, start_out : start_out + edge] = matrix
    high, low = in_two(both)
    return np.block([[high, low], [high, np.zeros_like(low)]])


def screened_kernel(grid_edge):
    signed = signed_points(grid_edge)
    row = np.zeros(lanes, np.int32)
    row[:grid_edge] = signed**2
    row[half : half + grid_edge] = signed**2
    pair = np.where(np.arange(lanes) < half, signed[0::2, None] ** 2, signed[1::2, None] ** 2) + row
    squared = jnp.asarray(pair, jnp.int32)[:, None, :] + jnp.asarray(signed**2, jnp.int32)[None, :, None]
    wave_sq = squared.astype(jnp.float32) * jnp.float32((2.0 * math.pi / cell_edge) ** 2)
    safe_sq = jnp.where(squared == 0, jnp.float32(1.0), wave_sq)
    screened = 4.0 * math.pi * -jnp.expm1(-safe_sq / (4.0 * screen_rate**2)) / safe_sq
    return jnp.where(squared == 0, jnp.float32(math.pi / screen_rate**2), screened)


def split(values):
    high = values.astype(jnp.bfloat16)
    low = (values - high.astype(jnp.float32)).astype(jnp.bfloat16)
    return high, low


def dot(left, right):
    return jnp.dot(left, right, preferred_element_type=jnp.float32)


def rows_products(table, slabs):
    done = []
    for first in range(0, len(slabs), 2):
        columns = []
        for slab in slabs[first : first + 2]:
            high, low = split(slab)
            columns.append(jnp.concatenate([high, low, high], axis=0))
        product = dot(table, jnp.concatenate(columns, axis=1))
        done += [product[:, k * lanes : (k + 1) * lanes] for k in range(len(columns))]
    return done


def lanes_product(slabs, table):
    high, low = split(jnp.concatenate(slabs, axis=0))
    return dot(jnp.concatenate([high, low], axis=1), table)


def lanes_result(product, count):
    edge = product.shape[0] // count
    product = product[:, :lanes] + product[:, lanes:]
    return [product[k * edge : (k + 1) * edge] for k in range(count)]


def in_stages(count, *stages):
    results = [()] * count
    for stage in stages:
        results = [(stage(i, *given),) for i, given in enumerate(results)]


def pair_kernel(grid_edge, slots, has_prior, last, *refs):
    refs = list(refs)
    home_ref, other_ref, kernel_ref = refs[:3]
    left_first_ref, left_fwd_ref, left_back_ref, left_last_ref, right_fwd_ref, right_back_ref = refs[3:9]
    prior_ref = refs[9] if has_prior else None
    outs = refs[9 + has_prior : -3 - last]
    work, back, turned = refs[-3 - last], refs[-2 - last], refs[-1 - last]
    result = refs[-1] if last else outs[0]

    me = lax.axis_index("off")
    line = 2 * grid_edge
    group = lanes // math.gcd(lanes, line)
    tiles = group * line // lanes
    pitch = work.shape[0] // (grid_edge // 2)
    planes = grid_edge // slots
    row_tiles = grid_edge * grid_edge // lanes
    lane = lax.broadcasted_iota(jnp.int32, (grid_edge, lanes), 1)
    together = 2 if grid_edge % 4 == 0 else 1
    in_first = lax.broadcasted_iota(jnp.int32, (grid_edge // 2, lanes), 1) < half

    def tiles_of(ref, block):
        first = block * tiles
        return [
            ref[:, (first + t) * lanes : (first + t + 1) * lanes].astype(jnp.float32)
            for t in range(tiles)
        ]

    def turn(values, amount):
        amount %= lanes
        return pltpu.roll(values, amount, 1) if amount else values

    def first_lanes(block):
        dense = [a * b for a, b in zip(tiles_of(home_ref, block), tiles_of(other_ref, block))]
        slabs = []
        for k in range(group):
            tile, offset = divmod(k * line, lanes)
            slab = dense[tile]
            if offset + line > lanes:
                slab = jnp.where(lane >= offset, slab, dense[tile + 1])
            slabs.append(turn(slab, -offset))
        return lanes_product(slabs, right_fwd_ref[...])

    def first_rows(block, product):
        return rows_products(left_first_ref[...], lanes_result(product, group))

    def first_store(block, slabs):
        for k, slab in enumerate(slabs):
            work[pl.ds((block * group + k) * pitch, grid_edge), :] = slab
            turned[pl.ds((block * group + k) * pitch, grid_edge), :] = turn(slab, half)

    in_stages(grid_edge // 2 // group, first_lanes, first_rows, first_store)

    def rows_of(block):
        start = 2 * block * together
        return [
            [pl.ds(start + 2 * k + d, grid_edge // 2, stride=pitch) for d in range(2)]
            for k in range(together)
        ]

    def middle_forward(block):
        slabs = []
        for pair in rows_of(block):
            even, odd = (work[r, :] for r in pair)
            turned_even, turned_odd = (turned[r, :] for r in pair)
            top = jnp.where(in_first, even, turned_odd)
            bottom = jnp.where(in_first, turned_even, odd)
            slabs.append(jnp.concatenate([top, bottom], axis=0))
        return rows_products(left_fwd_ref[...], slabs)

    def middle_back(block, slabs):
        slabs = [slab * kernel_ref[block * together + k] for k, slab in enumerate(slabs)]
        return rows_products(left_back_ref[...], slabs)

    def middle_store(block, slabs):
        for (row_even, row_odd), slab in zip(rows_of(block), slabs):
            top, bottom = slab[: grid_edge // 2], slab[grid_edge // 2 :]
            back[row_even, :] = jnp.where(in_first, top, turn(bottom, half))
            back[row_odd, :] = jnp.where(in_first, turn(top, half), bottom)

    in_stages(grid_edge // 2 // together, middle_forward, middle_back, middle_store)

    def last_rows(block):
        slabs = [back[pl.ds((block * group + k) * pitch, grid_edge), :] for k in range(group)]
        return rows_products(left_last_ref[...], slabs)

    def last_lanes(block, slabs):
        return lanes_product(slabs, right_back_ref[...])

    def last_store(block, product):
        slabs = [turn(slab, k * line) for k, slab in enumerate(lanes_result(product, group))]
        other = tiles_of(other_ref, block)
        for t in range(tiles):
            sources = range(t * lanes // line, ((t + 1) * lanes - 1) // line + 1)
            dense = slabs[sources[0]]
            for k in sources[1:]:
                dense = jnp.where(lane >= k * line - t * lanes, slabs[k], dense)
            total = dense * other[t]
            rows = pl.ds(block * tiles + t, planes, stride=row_tiles)
            for p in range(slots):
                result[me ^ p, rows, :] = total[p * planes : (p + 1) * planes]

    in_stages(grid_edge // 2 // group, last_rows, last_lanes, last_store)

    if last:
        for k in range(slots):
            terms = result[k]
            if has_prior:
                terms += prior_ref[k]
            outs[k % 4][k // 4] = terms
    elif has_prior:
        result[...] += prior_ref[...]


def pair_terms(slots, home, other, kernel, prior, last):
    grid_edge, plane_size = home.shape
    basis = real_basis(grid_edge)
    mixed = np.concatenate([np.arange(0, grid_edge, 2), np.arange(1, grid_edge, 2)])
    tables = (
        left_table(basis),
        left_table(basis[:, mixed]),
        left_table(basis.T[mixed]),
        left_table(-0.25 * basis.T),
        right_table(basis.T, grid_edge, half),
        right_table(basis, half, grid_edge),
    )
    slot_rows = grid_edge // slots * plane_size // lanes
    pitch = -(-grid_edge // 8) * 8 + 4
    whole = jax.ShapeDtypeStruct((slots, slot_rows, lanes), jnp.float32)
    part = jax.ShapeDtypeStruct((slots // 4, slot_rows, lanes), jnp.float32)
    vmem = pl.BlockSpec(memory_space=pltpu.VMEM)
    operands = [home, other, kernel, *(jnp.asarray(t) for t in tables)]
    operands += [] if prior is None else [prior]
    scratch = [pltpu.VMEM((grid_edge // 2 * pitch, lanes), jnp.float32)] * 3
    scratch += [pltpu.VMEM(whole.shape, jnp.float32)] if last else []
    return pl.pallas_call(
        functools.partial(pair_kernel, grid_edge, slots, prior is not None, last),
        out_shape=(part,) * 4 if last else whole,
        in_specs=[vmem] * len(operands),
        out_specs=(vmem,) * 4 if last else vmem,
        scratch_shapes=scratch,
        compiler_params=pltpu.CompilerParams(vmem_limit_bytes=32 * 1024 * 1024),
        cost_estimate=pl.CostEstimate(flops=10**9, bytes_accessed=2 * 10**6, transcendentals=0),
    )(*operands)


def fetch(block, cycle_size, groups):
    routes = ([], [])
    for source in range(cycle_size):
        for g in range(groups):
            for route, mask in zip(routes, (groups - 1 - g // 2, g // 2)):
                mask = cycle_size - 1 - mask if g % 2 else mask
                route.append((source * groups + g, (source ^ mask) * groups + g))
    first = lax.ppermute(block, ("blk", "off"), routes[0])
    second = lax.ppermute(block, ("blk", "off"), routes[1])
    return first, second


def scattered_sum(parts, groups):
    to_neighbour = [(g, g ^ 1) for g in range(groups)]
    passed_on = lax.ppermute(parts[3], "off", to_neighbour)
    kept = lax.ppermute(parts[1], "off", to_neighbour)
    near, far = parts[0] + kept, parts[2] + passed_on
    bit = 2
    while True:
        arrived = lax.ppermute(far, "off", [(g, g ^ bit) for g in range(groups)])
        near = near + arrived
        bit *= 2
        if bit == groups:
            return near[0]
        near, far = near[0::2], near[1::2]


def on_device(orbitals):
    band_count, grid_edge, plane_size = orbitals.shape
    cycle_size, groups = lax.axis_size("blk"), lax.axis_size("off")
    if cycle_size != 2 * groups or groups & (groups - 1) or groups < 4 or grid_edge > half:
        raise ValueError("unsupported mesh")
    first, second = fetch(orbitals, cycle_size, groups)
    kernel = screened_kernel(grid_edge)
    rows = []
    for home in orbitals:
        others = [*first, *second]
        terms = None
        for other in others[:-1]:
            terms = pair_terms(groups, home, other, kernel, terms, False)
        parts = pair_terms(groups, home, others[-1], kernel, terms, True)
        rows.append(scattered_sum(parts, groups))
    return jnp.stack(rows).reshape(band_count, grid_edge // groups, plane_size)


def solution(mesh):
    return jax.shard_map(
        on_device,
        mesh=mesh,
        in_specs=(P("blk", None, None),),
        out_specs=P("blk", "off", None),
        check_vma=False,
    )
```
